32 devices in a mesh: fsdp: 8 (over z, core), tp: 4 (over y, x).
Axes of the slice: x: 2, y: 2, z: 4, core: 2. Of those that a mesh axis runs over, the one named last changes fastest.
Arguments:
- hidden: bfloat16 [3072, 7168], P('fsdp'), may hold values from -72 to 72
- w_query: bfloat16 [7168, 4096], P('fsdp', 'tp'), may hold values from -0.0625 to 0.0625
- w_key: bfloat16 [7168, 1024], P('fsdp', 'tp'), may hold values from -0.0625 to 0.0625
- w_value: bfloat16 [7168, 1024], P('fsdp', 'tp'), may hold values from -0.0625 to 0.0625
- w_out: bfloat16 [4096, 7168], P('tp', 'fsdp'), may hold values from -0.09375 to 0.09375
- exp_query: int32 [56, 32], replicated, may hold values from -1 to 1
- exp_key: int32 [56, 8], replicated, may hold values from -1 to 1
- exp_value: int32 [56, 8], replicated, may hold values from -1 to 1
- exp_out: int32 [32, 56], replicated, may hold values from -1 to 1
- owner: int32 [8], replicated, may hold values from 0 to 7, each once
Outputs:
- attended: bfloat16 [3072, 7168], P('fsdp', 'tp')
The draws below stay inside these ranges and needn't reach their ends.
Inputs may be any that keep to these rules, and one draw needn't show every extreme that they name: Trainer shard i holds logical slab owner[i]; every slab is held once.
All inputs are finite; a program needn't handle non-finite values.
Results may differ from the reference program's by a relative error of at most 0.038.
Values may be sent and summed in bfloat16 or wider, within the bound.
A program may use at most 128 MiB of HBM per device.

```python
import math
import jax
import jax.numpy as jnp
from jax import lax

D = 7168
HQ = 32
HK = 8
HD = 128
BLOCK = 128
TOKENS = 3072
QW = 4096
KW = 1024
N_FSDP = 8
N_TP = 4


def draw_hidden(key, part):
    first = jax.random.fold_in(jax.random.fold_in(key, 17), 0)
    values = jnp.clip(jax.random.normal(first, (TOKENS, D), jnp.float32), -6.0, 6.0)
    return values.astype(jnp.bfloat16)


def with_ends(entries, stream_key, least, largest):
    longest = entries.shape.index(max(entries.shape))
    spots = []
    for shift in (0, 1):
        where = [jax.random.randint(jax.random.fold_in(stream_key, axis), (), 0, length) for axis, length in enumerate(entries.shape)]
        where[longest] = (where[longest] + shift) % entries.shape[longest]
        spots.append(tuple(where))
    return entries.at[spots[0]].set(least).at[spots[1]].set(largest)


def level_of(key, extent, cuts, smallest, top_value):
    factor_of, own = 1.0, jax.random.fold_in(key, 6)
    for axis_at, blocks in cuts:
        heights = jnp.exp(jax.random.uniform(jax.random.fold_in(own, axis_at), (blocks,), jnp.float32, smallest / len(cuts), top_value / len(cuts)))
        factor_of = factor_of * jnp.repeat(heights, extent[axis_at] // blocks).reshape([-1 if axis == axis_at else 1 for axis in range(len(extent))])
    return factor_of


def scatter_about(key, dims, spread, reach, pieces=(), held_as=jnp.bfloat16):
    entries = spread * jax.random.normal(key, dims, jnp.float32)
    if pieces:
        entries = entries * level_of(key, dims, pieces, -0.22, 0.18)
    return jnp.clip(entries, -reach, reach).astype(held_as)


def setup_inputs(seed: int = 0) -> dict:
    streams_of = jax.random.split(jax.random.key(seed), 11)
    hidden = draw_hidden(jax.random.fold_in(streams_of[10], 71), 0)
    w_query = scatter_about(streams_of[1], (D, QW), D ** -0.5, 0.0625, ((0, 8), (1, 4)))
    w_key = scatter_about(streams_of[2], (D, KW), D ** -0.5, 0.0625, ((0, 8), (1, 4)))
    w_value = scatter_about(streams_of[3], (D, KW), D ** -0.5, 0.0625, ((0, 8), (1, 4)))
    w_out = scatter_about(streams_of[4], (QW, D), QW ** -0.5, 0.09375, ((0, 4), (1, 8)))
    exp_query = with_ends(jax.random.randint(streams_of[5], (D // BLOCK, QW // BLOCK), -1, 2), jax.random.fold_in(streams_of[5], 1), -1, 1).astype(jnp.int32)
    exp_key = with_ends(jax.random.randint(streams_of[6], (D // BLOCK, KW // BLOCK), -1, 2), jax.random.fold_in(streams_of[6], 1), -1, 1).astype(jnp.int32)
    exp_value = with_ends(jax.random.randint(streams_of[7], (D // BLOCK, KW // BLOCK), -1, 2), jax.random.fold_in(streams_of[7], 1), -1, 1).astype(jnp.int32)
    exp_out = with_ends(jax.random.randint(streams_of[8], (QW // BLOCK, D // BLOCK), -1, 2), jax.random.fold_in(streams_of[8], 1), -1, 1).astype(jnp.int32)
    owner = jax.random.permutation(streams_of[9], N_FSDP).astype(jnp.int32)
    return dict(hidden=hidden, w_query=w_query, w_key=w_key, w_value=w_value, w_out=w_out, exp_query=exp_query, exp_key=exp_key, exp_value=exp_value, exp_out=exp_out, owner=owner)


neg_large = -1e+30

def dequantize(weight, exponents):
    block_size = weight.shape[0] // exponents.shape[0]
    factor = jnp.exp2(exponents.astype(jnp.float32))
    factor = jnp.repeat(jnp.repeat(factor, block_size, axis=0), block_size, axis=1)
    return (weight.astype(jnp.float32) * factor).astype(jnp.bfloat16)

def reference(hidden, w_query, w_key, w_value, w_out, exp_query, exp_key, exp_value, exp_out, owner):
    slab_rows = D // N_FSDP
    inverse = jnp.argsort(owner).astype(jnp.int32)

    def rows_logical(weight):
        shaped = weight.reshape(N_FSDP, slab_rows, weight.shape[1])
        return jnp.take(shaped, inverse, axis=0).reshape(weight.shape)

    def cols_logical(weight):
        shaped = weight.reshape(weight.shape[0], N_FSDP, slab_rows)
        return jnp.take(shaped, inverse, axis=1).reshape(weight.shape)
    query_w = dequantize(rows_logical(w_query), exp_query)
    key_w = dequantize(rows_logical(w_key), exp_key)
    value_w = dequantize(rows_logical(w_value), exp_value)
    out_w = dequantize(cols_logical(w_out), exp_out)
    query = jnp.dot(hidden, query_w, preferred_element_type=jnp.float32).astype(jnp.bfloat16)
    key_all = jnp.dot(hidden, key_w, preferred_element_type=jnp.float32).astype(jnp.bfloat16)
    value_all = jnp.dot(hidden, value_w, preferred_element_type=jnp.float32).astype(jnp.bfloat16)
    tokens = hidden.shape[0]
    group_size = HQ // HK
    query_heads = query.reshape(tokens, HQ, HD).transpose(1, 0, 2)
    key_heads = key_all.reshape(tokens, HK, HD).transpose(1, 0, 2)
    value_heads = value_all.reshape(tokens, HK, HD).transpose(1, 0, 2)
    position = jnp.arange(tokens, dtype=jnp.int32)
    causal = position[:, None] >= position[None, :]
    inv_root = 1.0 / math.sqrt(HD)

    def one_head(head_index):
        query_one = query_heads[head_index]
        key_one = key_heads[head_index // group_size]
        value_one = value_heads[head_index // group_size]
        scores = jnp.dot(query_one, key_one.T, preferred_element_type=jnp.float32) * inv_root
        scores = jnp.where(causal, scores, neg_large)
        row_top = lax.optimization_barrier(jnp.max(scores, axis=1, keepdims=True))
        weights = jnp.where(causal, jnp.exp(scores - row_top), 0.0)
        row_total = lax.optimization_barrier(jnp.sum(weights, axis=1, keepdims=True))
        mixed_sum = jnp.dot(weights.astype(jnp.bfloat16), value_one, preferred_element_type=jnp.float32)
        return (mixed_sum / row_total).astype(jnp.bfloat16)
    context = lax.map(one_head, jnp.arange(HQ, dtype=jnp.int32))
    context = context.transpose(1, 0, 2).reshape(tokens, HQ * HD)
    rows_tp = HQ * HD // N_TP
    attended = jnp.zeros((tokens, D), jnp.float32)
    for tp_rank in range(N_TP):
        part_sum = jnp.dot(context[:, tp_rank * rows_tp:(tp_rank + 1) * rows_tp], out_w[tp_rank * rows_tp:(tp_rank + 1) * rows_tp], preferred_element_type=jnp.float32)
        rounded = lax.optimization_barrier(part_sum.astype(jnp.bfloat16))
        attended = attended + rounded.astype(jnp.float32)
    return attended.astype(jnp.bfloat16)
```

```python
from functools import partial
import math

import jax
import jax.numpy as jnp
from jax import lax
from jax.experimental import pallas as pl
from jax.experimental.pallas import tpu as pltpu
from jax.sharding import PartitionSpec as P

HQ = 32
HK = 8
HD = 128


neg_large = -1e30


def block_factor(exponents, row_start, row_count, col_start, col_count, block_size):
    repeated = jnp.repeat(exponents, block_size, axis=0)
    picked = lax.dynamic_slice_in_dim(repeated, row_start, row_count, 0)
    repeated = jnp.repeat(picked, block_size, axis=1)
    picked = lax.dynamic_slice_in_dim(repeated, col_start, col_count, 1)
    return jnp.exp2(picked.astype(jnp.float32))


def block_update(state, query_half, pos_half, keys_part, values_part, key_pos, inv_root):
    row_max, row_sum, accum = state
    causal = pos_half[:, None] >= key_pos[None, :]
    scores = (
        jnp.einsum("tgjd,ngd->gjtn", query_half, keys_part, preferred_element_type=jnp.float32)
        * inv_root
    )
    scores = jnp.where(causal, scores, neg_large)
    new_max = jnp.maximum(row_max, jnp.max(scores, axis=3))
    rescale = jnp.exp(row_max - new_max)
    weights = jnp.where(causal, jnp.exp(scores - new_max[..., None]), 0.0)
    row_sum = row_sum * rescale + jnp.sum(weights, axis=3)
    accum = accum * rescale[..., None] + jnp.einsum(
        "gjtn,ngd->gjtd",
        weights.astype(jnp.bfloat16),
        values_part,
        preferred_element_type=jnp.float32,
    )
    return (new_max, row_sum, accum)


def keep_state(state):
    return state


def gather_body(hidden, w_query, w_key, w_value, w_out, exp_query, exp_key, exp_value, exp_out, owner):
    fsdp_index = lax.axis_index("fsdp")
    tp_index = lax.axis_index("tp")
    slab_rows = w_query.shape[0]
    groups = owner.shape[0]
    tokens = hidden.shape[0]
    model_width = hidden.shape[1]
    block_size = model_width // exp_query.shape[0]
    slab_start = owner[fsdp_index] * slab_rows
    query_cols = w_query.shape[1]
    key_cols = w_key.shape[1]

    def scaled_rows(weight, exponents):
        col_count = weight.shape[1]
        factor = block_factor(
            exponents, slab_start, slab_rows, tp_index * col_count, col_count, block_size
        )
        return (weight.astype(jnp.float32) * factor).astype(jnp.bfloat16)

    query_local = scaled_rows(w_query, exp_query)
    key_local = scaled_rows(w_key, exp_key)
    value_local = scaled_rows(w_value, exp_value)
    out_rows = w_out.shape[0]
    out_factor = block_factor(
        exp_out, tp_index * out_rows, out_rows, slab_start, slab_rows, block_size
    )
    out_local = (w_out.astype(jnp.float32) * out_factor).astype(jnp.bfloat16)
    arranged = jnp.take(hidden.reshape(tokens, groups, slab_rows), owner, axis=1).reshape(
        tokens, model_width
    )
    pieces = (
        lax.all_gather(query_local, "fsdp", axis=0, tiled=True),
        lax.all_gather(key_local, "fsdp", axis=0, tiled=True),
        lax.all_gather(value_local, "fsdp", axis=0, tiled=True),
    )
    query_sum, key_sum, value_sum = tuple(
        (jnp.dot(arranged, weight, preferred_element_type=jnp.float32) for weight in pieces)
    )
    query = query_sum.astype(jnp.bfloat16)
    key_here = key_sum.astype(jnp.bfloat16)
    value_here = value_sum.astype(jnp.bfloat16)
    half_rows = tokens // 2
    local_pos = fsdp_index * tokens + jnp.arange(tokens, dtype=jnp.int32)
    group_size = HQ // HK
    kv_heads = key_cols // HD
    query_halves = query.reshape(2, half_rows, kv_heads, group_size, HD)
    pos_halves = local_pos.reshape(2, half_rows)
    pos_top = jnp.max(pos_halves, axis=1)
    inv_root = 1.0 / math.sqrt(HD)
    one_state = (
        jnp.full((kv_heads, group_size, half_rows), neg_large, jnp.float32),
        jnp.zeros((kv_heads, group_size, half_rows), jnp.float32),
        jnp.zeros((kv_heads, group_size, half_rows, HD), jnp.float32),
    )
    offset = jnp.int32(0)
    key_piece = lax.all_gather(key_here, "fsdp", axis=0, tiled=True)
    value_piece = lax.all_gather(value_here, "fsdp", axis=0, tiled=True)
    states = list((one_state, one_state))
    piece_rows = key_piece.shape[0]
    for block_low in range(0, piece_rows, 1024):
        block_high = min(block_low + 1024, piece_rows)
        width_here = block_high - block_low
        keys_part = key_piece[block_low:block_high].reshape(width_here, kv_heads, HD)
        values_part = value_piece[block_low:block_high].reshape(width_here, kv_heads, HD)
        key_pos = offset + block_low + jnp.arange(width_here, dtype=jnp.int32)
        for attend_which in range(2):
            update = partial(
                block_update,
                query_half=query_halves[attend_which],
                pos_half=pos_halves[attend_which],
                keys_part=keys_part,
                values_part=values_part,
                key_pos=key_pos,
                inv_root=inv_root,
            )
            states[attend_which] = lax.cond(
                offset + block_low <= pos_top[attend_which],
                update,
                keep_state,
                states[attend_which],
            )
    final_states = tuple(states)
    context_parts = []
    for which in range(2):
        row_max, row_sum, accum = final_states[which]
        part_context = (accum / row_sum[..., None]).astype(jnp.bfloat16)
        context_parts.append(part_context.transpose(2, 0, 1, 3).reshape(half_rows, query_cols))
    context = jnp.concatenate(context_parts, axis=0)
    column_terms = jnp.dot(
        context,
        lax.all_gather(out_local, "fsdp", axis=1, tiled=True),
        preferred_element_type=jnp.float32,
    )
    slab_ids = jnp.arange(groups, dtype=jnp.int32)
    inverse = jnp.sum(
        slab_ids[:, None] * (owner[:, None] == slab_ids[None, :]).astype(jnp.int32), axis=0
    )
    ordered = jnp.take(column_terms.reshape(tokens, groups, slab_rows), inverse, axis=1).reshape(
        tokens, model_width
    )
    result = lax.psum_scatter(ordered.astype(jnp.bfloat16), "tp", scatter_dimension=1, tiled=True)
    return result


MESH = pl.DeviceIdType.MESH
VMEM = pltpu.VMEM
SMEM = pltpu.SMEM
DMA = pltpu.SemaphoreType.DMA
CORES = 2


def greet(peers):
    barrier = pltpu.get_barrier_semaphore()
    for device in peers:
        pl.semaphore_signal(barrier, inc=1, device_id=device, device_id_type=MESH)
    pl.semaphore_wait(barrier, len(peers))


def greet_all(n_f, n_t, f, t):
    greet(
        [{"fsdp": lax.rem(f + d, n_f)} for d in range(1, n_f)]
        + [{"tp": lax.rem(t + k, n_t)} for k in range(1, n_t)]
    )


def remote(src, dst, send, recv, device):
    return pltpu.make_async_remote_copy(
        src_ref=src,
        dst_ref=dst,
        send_sem=send,
        recv_sem=recv,
        device_id=device,
        device_id_type=MESH,
    )


def within(s, n):
    return jnp.logical_and(s >= 0, s < n)


def span_at(index, size):
    return pl.ds(pl.multiple_of(index * size, size), size)


def scale_into(out_ref, w_ref, fac_ref, at, blocks, block):
    for b in range(blocks):
        rows = slice(b * block, (b + 1) * block)
        for c in range(0, w_ref.shape[1], block):
            cols = slice(at + c, at + c + block)
            weight = w_ref[rows, c : c + block].astype(jnp.float32)
            out_ref[rows, cols] = (weight * fac_ref[b : b + 1, cols]).astype(jnp.bfloat16)


def head_kernel(
    n_f, n_t, share, block, pieces, pair_ref, wq_ref, wk_ref, wv_ref, fac_ref, q_ref, kv_ref,
    w_scr, hid, mine, px, up_in, down_in, acc,
    hid_send, hid_recv, side_send, pair_send, pair_recv,
    up_send, up_recv, down_send, down_recv, kv_send, kv_recv,
):
    f = lax.axis_index("fsdp")
    t = lax.axis_index("tp")
    n_z = n_f // CORES
    z, core = f // CORES, lax.rem(f, CORES)
    partner = z * CORES + (CORES - 1 - core)
    above, below = lax.rem(f + CORES, n_f), lax.rem(f - CORES + n_f, n_f)
    here = pair_ref.shape[1]
    slab = wq_ref.shape[0]
    quarter = here // n_t
    part = here // share
    q_cols, k_cols = wq_ref.shape[1], wk_ref.shape[1]
    blocks = slab // block
    side = [lax.rem(t + k, n_t) for k in range(n_t)]
    group, mate = f // share, lax.rem(f, share)

    def order(s):
        return lax.rem(s + n_f // 4, n_f)

    def piece_copy(i):
        rows = span_at(t, quarter)
        return remote(
            pieces.at[i], hid.at[f, rows], hid_send.at[i], hid_recv.at[f, t], {"fsdp": i}
        )

    def beside_copy():
        return remote(
            pair_ref.at[1], hid.at[f], hid_send.at[partner], hid_recv.at[f, 0], {"fsdp": partner}
        )

    def side_copy(b, k):
        rows = span_at(t, quarter)
        return remote(
            hid.at[b, rows], hid.at[b, rows], side_send.at[b, k], hid_recv.at[b, t], {"tp": side[k]}
        )

    def pair_copy(b):
        return remote(
            mine.at[b, CORES - 1 - core], px.at[b], pair_send.at[b], pair_recv.at[b],
            {"fsdp": partner},
        )

    def up_copy(b, zz):
        return remote(
            px.at[b, zz], up_in.at[b, zz], up_send.at[b, zz], up_recv.at[b, zz], {"fsdp": above}
        )

    def down_copy(b, zz):
        return remote(
            px.at[b, zz], down_in.at[b, zz], down_send.at[b, zz], down_recv.at[b, zz],
            {"fsdp": below},
        )

    def kv_copy(b, source, k):
        rows = pl.ds(pl.multiple_of(b * here + source * part, part), part)
        return remote(
            kv_ref.at[:, rows], kv_ref.at[:, rows], kv_send.at[b, k], kv_recv.at[b, source],
            {"fsdp": group * share + lax.rem(mate + k, share)},
        )

    greet_all(n_f, n_t, f, t)
    beside_copy().start()
    for d in range(1, n_z):
        for c in range(CORES):

            @pl.when(z + d < n_z)
            def _():
                piece_copy(lax.rem((z + d) * CORES + c, n_f)).start()

            @pl.when(z - d >= 0)
            def _():
                piece_copy(lax.rem((z - d + n_z) * CORES + c, n_f)).start()

    hid[f] = pair_ref[0]
    scale_into(w_scr, wq_ref, fac_ref, 0, blocks, block)
    scale_into(w_scr, wk_ref, fac_ref, q_cols, blocks, block)
    scale_into(w_scr, wv_ref, fac_ref, q_cols + k_cols, blocks, block)

    ahead = 2
    pair_lag = ahead + 1
    last_lag = ahead + n_z

    def step(s, carry):
        @pl.when(within(s, n_f))
        def _():
            b = order(s)

            @pl.when(b // CORES != z)
            def _():
                piece_like(b, t).wait_recv()
                for k in range(1, n_t):
                    side_copy(b, k).start()

        @pl.when(within(s - ahead, n_f))
        def _():
            b = order(s - ahead)

            @pl.when(b == partner)
            def _():
                remote(
                    pair_ref.at[1], hid.at[b], hid_send.at[0], hid_recv.at[b, 0], {"fsdp": partner}
                ).wait_recv()

            @pl.when(b // CORES != z)
            def _():
                for k in range(1, n_t):
                    piece_like(b, side[k]).wait_recv()

            both = jnp.dot(hid[b], w_scr[...], preferred_element_type=jnp.float32).astype(
                jnp.bfloat16
            )
            for j in range(n_f):
                g, p = j // share, j % share
                spot = mine.at[b, j % CORES, j // CORES]
                spot[:here, :] = both[:, j * HD : (j + 1) * HD]
                rows = slice(p * part, (p + 1) * part)
                k_at = q_cols + g * HD
                v_at = q_cols + k_cols + g * HD
                spot[here : here + part, :] = both[rows, k_at : k_at + HD]
                spot[here + part :, :] = both[rows, v_at : v_at + HD]
            pair_copy(b).start()

        @pl.when(within(s - pair_lag, n_f))
        def _():
            b = order(s - pair_lag)
            pair_copy(b).wait_recv()
            for zz in range(n_z):
                px[b, zz] = (
                    px[b, zz].astype(jnp.float32) + mine[b, core, zz].astype(jnp.float32)
                ).astype(jnp.bfloat16)

        up_at = s - pair_lag - z

        @pl.when(within(up_at, n_f))
        def _():
            b = order(up_at)
            for zz in range(n_z - 1, 0, -1):

                @pl.when(zz > z)
                def _():
                    @pl.when(z > 0)
                    def _():
                        up_copy(b, zz).wait_recv()
                        px[b, zz] = (
                            px[b, zz].astype(jnp.float32) + up_in[b, zz].astype(jnp.float32)
                        ).astype(jnp.bfloat16)

                    up_copy(b, zz).start()

        down_at = s - pair_lag - (n_z - 1 - z)

        @pl.when(within(down_at, n_f))
        def _():
            b = order(down_at)
            for zz in range(n_z - 1):

                @pl.when(zz < z)
                def _():
                    @pl.when(z < n_z - 1)
                    def _():
                        down_copy(b, zz).wait_recv()
                        px[b, zz] = (
                            px[b, zz].astype(jnp.float32) + down_in[b, zz].astype(jnp.float32)
                        ).astype(jnp.bfloat16)

                    down_copy(b, zz).start()

        @pl.when(within(s - last_lag, n_f))
        def _():
            b = order(s - last_lag)
            acc[...] = px[b, z].astype(jnp.float32)

            @pl.when(z > 0)
            def _():
                up_copy(b, z).wait_recv()
                acc[...] += up_in[b, z].astype(jnp.float32)

            @pl.when(z < n_z - 1)
            def _():
                down_copy(b, z).wait_recv()
                acc[...] += down_in[b, z].astype(jnp.float32)

            q_ref[span_at(b, here), :] = acc[:here, :].astype(jnp.bfloat16)
            rows = pl.ds(pl.multiple_of(b * here + mate * part, part), part)
            kv_ref[0, rows, :] = acc[here : here + part, :].astype(jnp.bfloat16)
            kv_ref[1, rows, :] = acc[here + part :, :].astype(jnp.bfloat16)
            for k in range(1, share):
                kv_copy(b, mate, k).start()

        return carry

    def piece_like(b, source):
        rows = span_at(source, quarter)
        return remote(
            pieces.at[0], hid.at[b, rows], hid_send.at[0], hid_recv.at[b, source], {"fsdp": above}
        )

    lax.fori_loop(0, n_f + last_lag, step, 0)

    def finish(b, carry):
        for k in range(1, share):
            kv_copy(b, lax.rem(mate - k + share, share), k).wait_recv()
            kv_copy(b, mate, k).wait_send()
        pair_copy(b).wait_send()

        @pl.when(b // CORES != z)
        def _():
            piece_copy(b).wait_send()
            for k in range(1, n_t):
                side_copy(b, k).wait_send()

        for zz in range(n_z):

            @pl.when(zz > z)
            def _():
                up_copy(b, zz).wait_send()

            @pl.when(zz < z)
            def _():
                down_copy(b, zz).wait_send()

        return carry

    lax.fori_loop(0, n_f, finish, 0)
    beside_copy().wait_send()


def arrange_kernel(n_f, owner_ref, place_ref, h_ref, pieces_ref, pair_ref, sem):
    quarter, slab = pieces_ref.shape[1], pieces_ref.shape[2]

    def columns(i):
        return pl.ds(pl.multiple_of(owner_ref[i] * slab, HD), slab)

    copies = []
    rows = pl.ds(pl.multiple_of(place_ref[0] * quarter, quarter), quarter)
    for k in range(2):
        source = h_ref.at[:, columns(place_ref[1 + k])]
        copies.append(pltpu.make_async_copy(source, pair_ref.at[k], sem.at[n_f + k]))
    for i in range(n_f):
        source = h_ref.at[rows, columns(i)]
        copies.append(pltpu.make_async_copy(source, pieces_ref.at[i], sem.at[i]))
    for copy in copies:
        copy.start()
    for copy in copies:
        copy.wait()


def arrange(n_f, n_t, slab, owner, hidden):
    f = lax.axis_index("fsdp")
    t = lax.axis_index("tp")
    here = hidden.shape[0]
    place = jnp.stack([t, f, f // CORES * CORES + (CORES - 1 - lax.rem(f, CORES))])
    whole = pl.BlockSpec(memory_space=VMEM)
    return pl.pallas_call(
        partial(arrange_kernel, n_f),
        out_shape=(
            jax.ShapeDtypeStruct((n_f, here // n_t, slab), hidden.dtype),
            jax.ShapeDtypeStruct((2, here, slab), hidden.dtype),
        ),
        in_specs=[pl.BlockSpec(memory_space=SMEM)] * 2 + [pl.BlockSpec(memory_space=pl.ANY)],
        out_specs=(whole, whole),
        scratch_shapes=[DMA((n_f + 2,))],
        name="arrange",
    )(owner, place, hidden)


def head(n_f, n_t, share, block, pieces, pair, w_query, w_key, w_value, factor):
    here = pair.shape[1]
    slab = w_query.shape[0]
    n_z = n_f // CORES
    cols = w_query.shape[1] + 2 * w_key.shape[1]
    packed = here + 2 * (here // share)
    tokens = here * n_f
    whole = pl.BlockSpec(memory_space=VMEM)
    return pl.pallas_call(
        partial(head_kernel, n_f, n_t, share, block),
        out_shape=(
            jax.ShapeDtypeStruct((tokens, HD), jnp.bfloat16),
            jax.ShapeDtypeStruct((2, tokens, HD), jnp.bfloat16),
        ),
        in_specs=[whole] * 6,
        out_specs=(whole, whole),
        scratch_shapes=[
            VMEM((slab, cols), jnp.bfloat16),
            VMEM((n_f, here, slab), jnp.bfloat16),
            VMEM((n_f, CORES, n_z, packed, HD), jnp.bfloat16),
            VMEM((n_f, n_z, packed, HD), jnp.bfloat16),
            VMEM((n_f, n_z, packed, HD), jnp.bfloat16),
            VMEM((n_f, n_z, packed, HD), jnp.bfloat16),
            VMEM((packed, HD), jnp.float32),
            DMA((n_f,)),
            DMA((n_f, n_t)),
            DMA((n_f, n_t)),
            DMA((n_f,)),
            DMA((n_f,)),
            DMA((n_f, n_z)),
            DMA((n_f, n_z)),
            DMA((n_f, n_z)),
            DMA((n_f, n_z)),
            DMA((n_f, share)),
            DMA((n_f, share)),
        ],
        compiler_params=pltpu.CompilerParams(
            collective_id=0, has_side_effects=True, vmem_limit_bytes=62 * 1024 * 1024
        ),
        name="project_and_sum",
    )(pieces, pair, w_query, w_key, w_value, factor)


def attend_kernel(inv_root, key_rows, q_ref, k_ref, v_ref, out_ref):
    i = pl.program_id(0)
    rows = q_ref.shape[0]
    query = q_ref[...]

    def step(j, state, masked):
        row_max, row_sum, accum = state
        at = pl.ds(pl.multiple_of(j * key_rows, key_rows), key_rows)
        scores = (
            lax.dot_general(
                query, k_ref[at, :], (((1,), (1,)), ((), ())), preferred_element_type=jnp.float32
            )
            * inv_root
        )
        if masked:
            q_pos = lax.broadcasted_iota(jnp.int32, scores.shape, 0)
            k_pos = lax.broadcasted_iota(jnp.int32, scores.shape, 1)
            scores = jnp.where(q_pos >= k_pos, scores, neg_large)
        new_max = jnp.maximum(row_max, jnp.max(scores, axis=1, keepdims=True))
        rescale = jnp.exp(row_max - new_max)
        weights = jnp.exp(scores - new_max)
        row_sum = row_sum * rescale + jnp.sum(weights, axis=1, keepdims=True)
        accum = accum * rescale + jnp.dot(
            weights.astype(jnp.bfloat16), v_ref[at, :], preferred_element_type=jnp.float32
        )
        return (new_max, row_sum, accum)

    state = (
        jnp.full((rows, 1), neg_large, jnp.float32),
        jnp.zeros((rows, 1), jnp.float32),
        jnp.zeros((rows, HD), jnp.float32),
    )
    state = step(i, state, True)
    _, row_sum, accum = lax.fori_loop(0, i, lambda j, s: step(j, s, False), state)
    out_ref[...] = (accum / row_sum).astype(jnp.bfloat16)


def tail_kernel(
    n_f, n_t, block, inverse_ref, c_ref, w_ref, fac_ref, out_ref,
    w_scr, ctx, y, got, total, slabs, fin,
    line_send, line_recv, sum_send, sum_recv, slab_send, slab_recv, last_send, last_recv,
):
    f = lax.axis_index("fsdp")
    t = lax.axis_index("tp")
    n_z = n_f // CORES
    z, core = f // CORES, lax.rem(f, CORES)
    partner = z * CORES + (CORES - 1 - core)
    above, below = lax.rem(f + CORES, n_f), lax.rem(f - CORES + n_f, n_f)
    here = c_ref.shape[0] // n_f
    slab = w_ref.shape[1]
    quarter = here // n_t
    per = n_f // n_t
    blocks = w_ref.shape[0] // block
    side = [lax.rem(t + k, n_t) for k in range(n_t)]

    def order(s):
        return lax.rem(s * 3, n_f)

    def line_copy(i, zz, to, which):
        rows = span_at(i, here)
        h = lax.rem(zz + n_z, n_z) * CORES + core
        return remote(
            ctx.at[h, rows], ctx.at[h, rows], line_send.at[i, h // CORES, which],
            line_recv.at[i, h], {"fsdp": to},
        )

    def line_wait(i, h):
        rows = span_at(i, here)
        remote(
            ctx.at[h, rows], ctx.at[h, rows], line_send.at[i, 0, 0], line_recv.at[i, h],
            {"fsdp": partner},
        ).wait_recv()

    def sum_copy(i, k):
        return remote(
            y.at[i, side[k]], got.at[i, k - 1], sum_send.at[i, k - 1], sum_recv.at[i, k - 1],
            {"tp": side[k]},
        )

    def slab_copy(i):
        return remote(total.at[i], slabs.at[f], slab_send.at[i], slab_recv.at[f], {"fsdp": i})

    def last_copy(k):
        return remote(
            fin.at[side[k]], out_ref.at[span_at(t, quarter)], last_send.at[k - 1],
            last_recv.at[k - 1], {"tp": side[k]},
        )

    ctx[f] = c_ref[...]
    w_scr[...] = jnp.zeros_like(w_scr)
    scale_into(w_scr, w_ref, fac_ref, 0, blocks, block)
    greet_all(n_f, n_t, f, t)

    def relay(s, d):
        @pl.when(within(s - d, n_f))
        def _():
            i = order(s - d)

            @pl.when(z - d >= 0)
            def _():
                zz = lax.rem(z - d + n_z, n_z)
                line_wait(i, zz * CORES + core)

                @pl.when(z < n_z - 1)
                def _():
                    line_copy(i, zz, above, 1).start()

                line_copy(i, zz, partner, 0).start()

            @pl.when(z + d < n_z)
            def _():
                zz = lax.rem(z + d, n_z)
                line_wait(i, zz * CORES + core)

                @pl.when(z > 0)
                def _():
                    line_copy(i, zz, below, 2).start()

                line_copy(i, zz, partner, 0).start()

    def step(s, carry):
        @pl.when(within(s, n_f))
        def _():
            i = order(s)

            @pl.when(z < n_z - 1)
            def _():
                line_copy(i, z, above, 1).start()

            @pl.when(z > 0)
            def _():
                line_copy(i, z, below, 2).start()

            line_copy(i, z, partner, 0).start()

        for d in range(1, n_z):
            relay(s, d)

        @pl.when(within(s - n_z, n_f))
        def _():
            i = order(s - n_z)
            for zz in range(n_z):
                line_wait(i, zz * CORES + (CORES - 1 - core))
            context = jnp.concatenate([ctx[h, span_at(i, here)] for h in range(n_f)], axis=1)
            part = jnp.dot(context, w_scr[...], preferred_element_type=jnp.float32).astype(
                jnp.bfloat16
            )
            for r in range(n_t):
                y[i, r] = part[r * quarter : (r + 1) * quarter, :slab]
            for k in range(1, n_t):
                sum_copy(i, k).start()

        @pl.when(within(s - n_z - 1, n_f))
        def _():
            i = order(s - n_z - 1)
            summed = y[i, t].astype(jnp.float32)
            for k in range(1, n_t):
                sum_copy(i, k).wait_recv()
                summed = summed + got[i, k - 1].astype(jnp.float32)
            total[i] = summed.astype(jnp.bfloat16)

            @pl.when(i == f)
            def _():
                slabs[i] = total[i]

            @pl.when(i != f)
            def _():
                slab_copy(i).start()

        return carry

    lax.fori_loop(0, n_f + n_z + 1, step, 0)

    for d in range(1, n_f):
        source = lax.rem(f + d, n_f)
        remote(
            total.at[0], slabs.at[source], slab_send.at[0], slab_recv.at[source], {"fsdp": source}
        ).wait_recv()
    for j in range(n_f):
        fin[j // per, :, (j % per) * slab : (j % per + 1) * slab] = slabs[inverse_ref[j]]
    for k in range(1, n_t):
        last_copy(k).start()
    out_ref[span_at(t, quarter), :] = fin[t]

    def finish(i, carry):
        @pl.when(i != f)
        def _():
            slab_copy(i).wait_send()

        for k in range(1, n_t):
            sum_copy(i, k).wait_send()
        for zz in range(n_z):
            line_copy(i, zz, partner, 0).wait_send()

            @pl.when(jnp.logical_and(zz <= z, z < n_z - 1))
            def _():
                line_copy(i, zz, above, 1).wait_send()

            @pl.when(jnp.logical_and(zz >= z, z > 0))
            def _():
                line_copy(i, zz, below, 2).wait_send()

        return carry

    lax.fori_loop(0, n_f, finish, 0)
    for k in range(1, n_t):
        source = lax.rem(t - k + n_t, n_t)
        remote(
            fin.at[0], out_ref.at[span_at(source, quarter)], last_send.at[k - 1],
            last_recv.at[k - 1], {"tp": side[1]},
        ).wait_recv()
        last_copy(k).wait_send()


def tail(n_f, n_t, block, inverse, context, w_out, factor):
    tokens = context.shape[0]
    here = tokens // n_f
    quarter = here // n_t
    slab = w_out.shape[1]
    wide = slab * n_f // n_t
    n_z = n_f // CORES
    whole = pl.BlockSpec(memory_space=VMEM)
    return pl.pallas_call(
        partial(tail_kernel, n_f, n_t, block),
        out_shape=jax.ShapeDtypeStruct((here, wide), jnp.bfloat16),
        in_specs=[pl.BlockSpec(memory_space=SMEM)] + [whole] * 3,
        out_specs=whole,
        scratch_shapes=[
            VMEM((w_out.shape[0], slab + -slab % 256), jnp.bfloat16),
            VMEM((n_f, tokens, HD), jnp.bfloat16),
            VMEM((n_f, n_t, quarter, slab), jnp.bfloat16),
            VMEM((n_f, n_t - 1, quarter, slab), jnp.bfloat16),
            VMEM((n_f, quarter, slab), jnp.bfloat16),
            VMEM((n_f, quarter, slab), jnp.bfloat16),
            VMEM((n_t, quarter, wide), jnp.bfloat16),
            DMA((n_f, n_z, 3)),
            DMA((n_f, n_f)),
            DMA((n_f, n_t - 1)),
            DMA((n_f, n_t - 1)),
            DMA((n_f,)),
            DMA((n_f,)),
            DMA((n_t - 1,)),
            DMA((n_t - 1,)),
        ],
        compiler_params=pltpu.CompilerParams(
            collective_id=1, has_side_effects=True, vmem_limit_bytes=56 * 1024 * 1024
        ),
        name="project_out_and_sum",
    )(inverse, context, w_out, factor)


def stationary_body(
    n_f, n_t, hidden, w_query, w_key, w_value, w_out, exp_query, exp_key, exp_value, exp_out, owner
):
    f = lax.axis_index("fsdp")
    t = lax.axis_index("tp")
    here, width = hidden.shape
    slab = w_query.shape[0]
    tokens = here * n_f
    block = width // exp_query.shape[0]
    slab_blocks = slab // block
    q_cols, k_cols = w_query.shape[1], w_key.shape[1]
    share = (q_cols // HD) // (k_cols // HD)
    logical = owner[f]

    def factors(exponents, cols):
        picked = lax.dynamic_slice(
            exponents, (logical * slab_blocks, t * (cols // block)), (slab_blocks, cols // block)
        )
        return jnp.repeat(jnp.exp2(picked.astype(jnp.float32)), block, axis=1)

    in_factor = jnp.concatenate(
        [factors(exp_query, q_cols), factors(exp_key, k_cols), factors(exp_value, k_cols)], axis=1
    )
    out_rows = w_out.shape[0] // block
    out_factor = jnp.repeat(
        jnp.exp2(
            lax.dynamic_slice(
                exp_out, (t * out_rows, logical * slab_blocks), (out_rows, slab_blocks)
            ).astype(jnp.float32)
        ),
        block,
        axis=1,
    )
    in_factor = jnp.pad(in_factor, ((0, -slab_blocks % 8), (0, 0)))
    out_factor = jnp.pad(out_factor, ((0, -out_rows % 8), (0, -slab % 256)))

    pieces, pair = arrange(n_f, n_t, slab, owner, hidden)
    query, kv = head(
        n_f, n_t, share, block, pieces, pair, w_query, w_key, w_value, in_factor
    )
    tile = here
    context = pl.pallas_call(
        partial(attend_kernel, 1.0 / math.sqrt(HD), tile),
        grid=(tokens // tile,),
        out_shape=jax.ShapeDtypeStruct((tokens, HD), jnp.bfloat16),
        in_specs=[
            pl.BlockSpec((tile, HD), lambda i: (i, 0)),
            pl.BlockSpec((pl.squeezed, tokens, HD), lambda i: (0, 0, 0)),
            pl.BlockSpec((pl.squeezed, tokens, HD), lambda i: (1, 0, 0)),
        ],
        out_specs=pl.BlockSpec((tile, HD), lambda i: (i, 0)),
        compiler_params=pltpu.CompilerParams(vmem_limit_bytes=48 * 1024 * 1024),
        name="attend",
    )(query, kv, kv)

    slab_ids = jnp.arange(n_f, dtype=jnp.int32)
    inverse = jnp.sum(
        slab_ids[:, None] * (owner[:, None] == slab_ids[None, :]).astype(jnp.int32), axis=0
    )
    return tail(n_f, n_t, block, inverse, context, w_out, out_factor)


def solution(mesh):
    n_f, n_t = mesh.shape["fsdp"], mesh.shape["tp"]

    def body(*arrays):
        hidden, w_query, w_key = arrays[0], arrays[1], arrays[2]
        heads, kv_heads = w_query.shape[1] // HD, w_key.shape[1] // HD
        share = heads // kv_heads
        fits = (
            heads == n_f
            and n_f % n_t == 0
            and n_f % CORES == 0
            and hidden.shape[0] % (16 * n_t) == 0
            and hidden.shape[0] % (16 * share) == 0
        )
        if fits:
            return stationary_body(n_f, n_t, *arrays)
        return gather_body(*arrays)

    placed = (
        P("fsdp", None),
        P("fsdp", "tp"),
        P("fsdp", "tp"),
        P("fsdp", "tp"),
        P("tp", "fsdp"),
        P(),
        P(),
        P(),
        P(),
        P(),
    )
    return jax.shard_map(
        body, mesh=mesh, in_specs=placed, out_specs=P("fsdp", "tp"), check_vma=False
    )
```

```python
from functools import partial
import math

import jax
import jax.numpy as jnp
from jax import lax
from jax.experimental import pallas as pl
from jax.experimental.pallas import tpu as pltpu
from jax.sharding import PartitionSpec as P

HQ = 32
HK = 8
HD = 128


neg_large = -1e30


def block_factor(exponents, row_start, row_count, col_start, col_count, block_size):
    repeated = jnp.repeat(exponents, block_size, axis=0)
    picked = lax.dynamic_slice_in_dim(repeated, row_start, row_count, 0)
    repeated = jnp.repeat(picked, block_size, axis=1)
    picked = lax.dynamic_slice_in_dim(repeated, col_start, col_count, 1)
    return jnp.exp2(picked.astype(jnp.float32))


def block_update(state, query_half, pos_half, keys_part, values_part, key_pos, inv_root):
    row_max, row_sum, accum = state
    causal = pos_half[:, None] >= key_pos[None, :]
    scores = (
        jnp.einsum("tgjd,ngd->gjtn", query_half, keys_part, preferred_element_type=jnp.float32)
        * inv_root
    )
    scores = jnp.where(causal, scores, neg_large)
    new_max = jnp.maximum(row_max, jnp.max(scores, axis=3))
    rescale = jnp.exp(row_max - new_max)
    weights = jnp.where(causal, jnp.exp(scores - new_max[..., None]), 0.0)
    row_sum = row_sum * rescale + jnp.sum(weights, axis=3)
    accum = accum * rescale[..., None] + jnp.einsum(
        "gjtn,ngd->gjtd",
        weights.astype(jnp.bfloat16),
        values_part,
        preferred_element_type=jnp.float32,
    )
    return (new_max, row_sum, accum)


def keep_state(state):
    return state


def gather_body(hidden, w_query, w_key, w_value, w_out, exp_query, exp_key, exp_value, exp_out, owner):
    fsdp_index = lax.axis_index("fsdp")
    tp_index = lax.axis_index("tp")
    slab_rows = w_query.shape[0]
    groups = owner.shape[0]
    tokens = hidden.shape[0]
    model_width = hidden.shape[1]
    block_size = model_width // exp_query.shape[0]
    slab_start = owner[fsdp_index] * slab_rows
    query_cols = w_query.shape[1]
    key_cols = w_key.shape[1]

    def scaled_rows(weight, exponents):
        col_count = weight.shape[1]
        factor = block_factor(
            exponents, slab_start, slab_rows, tp_index * col_count, col_count, block_size
        )
        return (weight.astype(jnp.float32) * factor).astype(jnp.bfloat16)

    query_local = scaled_rows(w_query, exp_query)
    key_local = scaled_rows(w_key, exp_key)
    value_local = scaled_rows(w_value, exp_value)
    out_rows = w_out.shape[0]
    out_factor = block_factor(
        exp_out, tp_index * out_rows, out_rows, slab_start, slab_rows, block_size
    )
    out_local = (w_out.astype(jnp.float32) * out_factor).astype(jnp.bfloat16)
    arranged = jnp.take(hidden.reshape(tokens, groups, slab_rows), owner, axis=1).reshape(
        tokens, model_width
    )
    pieces = (
        lax.all_gather(query_local, "fsdp", axis=0, tiled=True),
        lax.all_gather(key_local, "fsdp", axis=0, tiled=True),
        lax.all_gather(value_local, "fsdp", axis=0, tiled=True),
    )
    query_sum, key_sum, value_sum = tuple(
        (jnp.dot(arranged, weight, preferred_element_type=jnp.float32) for weight in pieces)
    )
    query = query_sum.astype(jnp.bfloat16)
    key_here = key_sum.astype(jnp.bfloat16)
    value_here = value_sum.astype(jnp.bfloat16)
    half_rows = tokens // 2
    local_pos = fsdp_index * tokens + jnp.arange(tokens, dtype=jnp.int32)
    group_size = HQ // HK
    kv_heads = key_cols // HD
    query_halves = query.reshape(2, half_rows, kv_heads, group_size, HD)
    pos_halves = local_pos.reshape(2, half_rows)
    pos_top = jnp.max(pos_halves, axis=1)
    inv_root = 1.0 / math.sqrt(HD)
    one_state = (
        jnp.full((kv_heads, group_size, half_rows), neg_large, jnp.float32),
        jnp.zeros((kv_heads, group_size, half_rows), jnp.float32),
        jnp.zeros((kv_heads, group_size, half_rows, HD), jnp.float32),
    )
    offset = jnp.int32(0)
    key_piece = lax.all_gather(key_here, "fsdp", axis=0, tiled=True)
    value_piece = lax.all_gather(value_here, "fsdp", axis=0, tiled=True)
    states = list((one_state, one_state))
    piece_rows = key_piece.shape[0]
    for block_low in range(0, piece_rows, 1024):
        block_high = min(block_low + 1024, piece_rows)
        width_here = block_high - block_low
        keys_part = key_piece[block_low:block_high].reshape(width_here, kv_heads, HD)
        values_part = value_piece[block_low:block_high].reshape(width_here, kv_heads, HD)
        key_pos = offset + block_low + jnp.arange(width_here, dtype=jnp.int32)
        for attend_which in range(2):
            update = partial(
                block_update,
                query_half=query_halves[attend_which],
                pos_half=pos_halves[attend_which],
                keys_part=keys_part,
                values_part=values_part,
                key_pos=key_pos,
                inv_root=inv_root,
            )
            states[attend_which] = lax.cond(
                offset + block_low <= pos_top[attend_which],
                update,
                keep_state,
                states[attend_which],
            )
    final_states = tuple(states)
    context_parts = []
    for which in range(2):
        row_max, row_sum, accum = final_states[which]
        part_context = (accum / row_sum[..., None]).astype(jnp.bfloat16)
        context_parts.append(part_context.transpose(2, 0, 1, 3).reshape(half_rows, query_cols))
    context = jnp.concatenate(context_parts, axis=0)
    column_terms = jnp.dot(
        context,
        lax.all_gather(out_local, "fsdp", axis=1, tiled=True),
        preferred_element_type=jnp.float32,
    )
    slab_ids = jnp.arange(groups, dtype=jnp.int32)
    inverse = jnp.sum(
        slab_ids[:, None] * (owner[:, None] == slab_ids[None, :]).astype(jnp.int32), axis=0
    )
    ordered = jnp.take(column_terms.reshape(tokens, groups, slab_rows), inverse, axis=1).reshape(
        tokens, model_width
    )
    result = lax.psum_scatter(ordered.astype(jnp.bfloat16), "tp", scatter_dimension=1, tiled=True)
    return result


MESH = pl.DeviceIdType.MESH
VMEM = pltpu.VMEM
SMEM = pltpu.SMEM
DMA = pltpu.SemaphoreType.DMA
CORES = 2
LINE = 4
SIDE = 2


def greet(peers):
    barrier = pltpu.get_barrier_semaphore()
    for device in peers:
        pl.semaphore_signal(barrier, inc=1, device_id=device, device_id_type=MESH)
    pl.semaphore_wait(barrier, len(peers))


def greet_all(n_f, n_t, f, t):
    greet(
        [{"fsdp": lax.rem(f + d, n_f)} for d in range(1, n_f)]
        + [{"tp": lax.rem(t + k, n_t)} for k in range(1, n_t)]
    )


def remote(src, dst, send, recv, device):
    return pltpu.make_async_remote_copy(
        src_ref=src,
        dst_ref=dst,
        send_sem=send,
        recv_sem=recv,
        device_id=device,
        device_id_type=MESH,
    )


def within(s, n):
    return jnp.logical_and(s >= 0, s < n)


def span_at(index, size):
    return pl.ds(pl.multiple_of(index * size, size), size)


def scale_into(out_ref, w_ref, fac_ref, at, blocks, block):
    for b in range(blocks):
        rows = slice(b * block, (b + 1) * block)
        for c in range(0, w_ref.shape[1], block):
            cols = slice(at + c, at + c + block)
            weight = w_ref[rows, c : c + block].astype(jnp.float32)
            out_ref[rows, cols] = (weight * fac_ref[b : b + 1, cols]).astype(jnp.bfloat16)


def head_kernel(
    n_f, n_t, share, block, pieces, pair_ref, wq_ref, wk_ref, wv_ref, fac_ref, q_ref, kv_ref,
    w_scr, hid, mine, px, up_in, down_in, acc,
    hid_send, hid_recv, side_send, pair_send, pair_recv,
    up_send, up_recv, down_send, down_recv, kv_send, kv_recv,
):
    f = lax.axis_index("fsdp")
    t = lax.axis_index("tp")
    n_z = n_f // CORES
    z, core = f // CORES, lax.rem(f, CORES)
    partner = z * CORES + (CORES - 1 - core)
    above, below = lax.rem(f + CORES, n_f), lax.rem(f - CORES + n_f, n_f)
    here = pair_ref.shape[1]
    slab = wq_ref.shape[0]
    quarter = here // n_t
    part = here // share
    q_cols, k_cols = wq_ref.shape[1], wk_ref.shape[1]
    blocks = slab // block
    side = [lax.rem(t + k, n_t) for k in range(n_t)]
    group, mate = f // share, lax.rem(f, share)

    middle = 1 - (z == 0).astype(jnp.int32) - (z == n_z - 1).astype(jnp.int32)
    upper = z // (n_z // 2)

    def turned(b):
        return b + upper * (n_f - 1 - 2 * b)

    def piece_copy(i):
        rows = span_at(t, quarter)
        return remote(
            pieces.at[i], hid.at[f, rows], hid_send.at[i], hid_recv.at[f, t], {"fsdp": i}
        )

    def beside_copy():
        return remote(
            pair_ref.at[1], hid.at[f], hid_send.at[partner], hid_recv.at[f, 0], {"fsdp": partner}
        )

    def side_copy(b, k):
        rows = span_at(t, quarter)
        return remote(
            hid.at[b, rows], hid.at[b, rows], side_send.at[b, k], hid_recv.at[b, t], {"tp": side[k]}
        )

    def pair_copy(b):
        return remote(
            mine.at[b, CORES - 1 - core], px.at[b], pair_send.at[b], pair_recv.at[b],
            {"fsdp": partner},
        )

    def up_copy(b, zz):
        return remote(
            px.at[b, zz], up_in.at[b, zz], up_send.at[b, zz], up_recv.at[b, zz], {"fsdp": above}
        )

    def down_copy(b, zz):
        return remote(
            px.at[b, zz], down_in.at[b, zz], down_send.at[b, zz], down_recv.at[b, zz],
            {"fsdp": below},
        )

    def kv_copy(b, source, k):
        rows = pl.ds(pl.multiple_of(b * here + source * part, part), part)
        return remote(
            kv_ref.at[:, rows], kv_ref.at[:, rows], kv_send.at[b, k], kv_recv.at[b, source],
            {"fsdp": group * share + lax.rem(mate + k, share)},
        )

    greet_all(n_f, n_t, f, t)
    beside_copy().start()
    for d in range(1, n_z):
        for c in range(CORES):

            @pl.when(z + d < n_z)
            def _():
                piece_copy(lax.rem((z + d) * CORES + c, n_f)).start()

            @pl.when(z - d >= 0)
            def _():
                piece_copy(lax.rem((z - d + n_z) * CORES + c, n_f)).start()

    hid[f] = pair_ref[0]
    scale_into(w_scr, wq_ref, fac_ref, 0, blocks, block)
    scale_into(w_scr, wk_ref, fac_ref, q_cols, blocks, block)
    scale_into(w_scr, wv_ref, fac_ref, q_cols + k_cols, blocks, block)

    def piece_like(b, source):
        rows = span_at(source, quarter)
        return remote(
            pieces.at[0], hid.at[b, rows], hid_send.at[0], hid_recv.at[b, source], {"fsdp": above}
        )

    def pass_on(b):
        piece_like(b, t).wait_recv()
        for k in range(1, n_t):
            side_copy(b, k).start()

    def project(b):
        @pl.when(b == partner)
        def _():
            remote(
                pair_ref.at[1], hid.at[b], hid_send.at[0], hid_recv.at[b, 0], {"fsdp": partner}
            ).wait_recv()

        @pl.when(b // CORES != z)
        def _():
            for k in range(1, n_t):
                piece_like(b, side[k]).wait_recv()

        both = jnp.dot(hid[b], w_scr[...], preferred_element_type=jnp.float32).astype(
            jnp.bfloat16
        )
        for j in range(n_f):
            g, p = j // share, j % share
            spot = mine.at[b, j % CORES, j // CORES]
            spot[:here, :] = both[:, j * HD : (j + 1) * HD]
            rows = slice(p * part, (p + 1) * part)
            k_at = q_cols + g * HD
            v_at = q_cols + k_cols + g * HD
            spot[here : here + part, :] = both[rows, k_at : k_at + HD]
            spot[here + part :, :] = both[rows, v_at : v_at + HD]
        pair_copy(b).start()

    def join_pair(b):
        pair_copy(b).wait_recv()
        for zz in range(n_z):
            px[b, zz] = (
                px[b, zz].astype(jnp.float32) + mine[b, core, zz].astype(jnp.float32)
            ).astype(jnp.bfloat16)

    def first_slot(s, work):
        at = s - middle

        @pl.when(within(at, n_f - middle * (n_f // 2)))
        def _():
            work(turned(at))

    def second_slot(s, work):
        at = s - 2

        @pl.when(jnp.logical_and(middle == 1, within(at, n_f // 2)))
        def _():
            work(turned(n_f - 1 - at))

    def close(b):
        acc[...] = px[b, z].astype(jnp.float32)

        @pl.when(z > 0)
        def _():
            up_copy(b, z).wait_recv()
            acc[...] += up_in[b, z].astype(jnp.float32)

        @pl.when(z < n_z - 1)
        def _():
            down_copy(b, z).wait_recv()
            acc[...] += down_in[b, z].astype(jnp.float32)

        q_ref[span_at(b, here), :] = acc[:here, :].astype(jnp.bfloat16)
        rows = pl.ds(pl.multiple_of(b * here + mate * part, part), part)
        kv_ref[0, rows, :] = acc[here : here + part, :].astype(jnp.bfloat16)
        kv_ref[1, rows, :] = acc[here + part :, :].astype(jnp.bfloat16)
        for k in range(1, share):
            kv_copy(b, mate, k).start()

    @pl.when(middle == 1)
    def _():
        for c in range(CORES):
            pass_on(turned(c))
        for c in range(CORES):
            pass_on(turned(3 * CORES - 1 - c))

    def step(s, carry):
        first_slot(s, project)
        second_slot(s, project)

        @pl.when(jnp.logical_and(middle == 0, within(s, n_f - CORES)))
        def _():
            pass_on(turned(s + CORES))

        @pl.when(jnp.logical_and(middle == 1, s == 1))
        def _():
            for c in range(CORES):
                pass_on(turned(n_f - 1 - c))

        first_slot(s - 1, join_pair)
        second_slot(s - 1, join_pair)

        up_at = s - 1 - z

        @pl.when(within(up_at, n_f))
        def _():
            b = up_at
            for zz in range(n_z - 1, 0, -1):

                @pl.when(zz > z)
                def _():
                    @pl.when(z > 0)
                    def _():
                        up_copy(b, zz).wait_recv()
                        px[b, zz] = (
                            px[b, zz].astype(jnp.float32) + up_in[b, zz].astype(jnp.float32)
                        ).astype(jnp.bfloat16)

                    up_copy(b, zz).start()

        down_at = s - 1 - (n_z - 1 - z)

        @pl.when(within(down_at, n_f))
        def _():
            b = n_f - 1 - down_at
            for zz in range(n_z - 1):

                @pl.when(zz < z)
                def _():
                    @pl.when(z < n_z - 1)
                    def _():
                        down_copy(b, zz).wait_recv()
                        px[b, zz] = (
                            px[b, zz].astype(jnp.float32) + down_in[b, zz].astype(jnp.float32)
                        ).astype(jnp.bfloat16)

                    down_copy(b, zz).start()

        one = middle * (n_f + 2 - s) + (1 - middle) * (n_f - 1 - 2 * (s - n_f))
        first_close = n_f - 2 * middle

        @pl.when(jnp.logical_and(s >= first_close, one >= 0))
        def _():
            close(turned(one))

        two = middle * (s - 2) + (1 - middle) * (one - 1)

        @pl.when(
            jnp.logical_and(s >= first_close + middle, jnp.logical_and(two >= 0, two < n_f))
        )
        def _():
            close(turned(two))

        return carry

    lax.fori_loop(0, n_f + n_z, step, 0)

    def finish(b, carry):
        for k in range(1, share):
            kv_copy(b, lax.rem(mate - k + share, share), k).wait_recv()
            kv_copy(b, mate, k).wait_send()
        pair_copy(b).wait_send()

        @pl.when(b // CORES != z)
        def _():
            piece_copy(b).wait_send()
            for k in range(1, n_t):
                side_copy(b, k).wait_send()

        for zz in range(n_z):

            @pl.when(zz > z)
            def _():
                up_copy(b, zz).wait_send()

            @pl.when(zz < z)
            def _():
                down_copy(b, zz).wait_send()

        return carry

    lax.fori_loop(0, n_f, finish, 0)
    beside_copy().wait_send()


def arrange_kernel(n_f, owner_ref, place_ref, h_ref, pieces_ref, pair_ref, sem):
    quarter, slab = pieces_ref.shape[1], pieces_ref.shape[2]

    def columns(i):
        return pl.ds(pl.multiple_of(owner_ref[i] * slab, HD), slab)

    copies = []
    rows = pl.ds(pl.multiple_of(place_ref[0] * quarter, quarter), quarter)
    for k in range(2):
        source = h_ref.at[:, columns(place_ref[1 + k])]
        copies.append(pltpu.make_async_copy(source, pair_ref.at[k], sem.at[n_f + k]))
    for i in range(n_f):
        source = h_ref.at[rows, columns(i)]
        copies.append(pltpu.make_async_copy(source, pieces_ref.at[i], sem.at[i]))
    for copy in copies:
        copy.start()
    for copy in copies:
        copy.wait()


def arrange(n_f, n_t, slab, owner, hidden):
    f = lax.axis_index("fsdp")
    t = lax.axis_index("tp")
    here = hidden.shape[0]
    place = jnp.stack([t, f, f // CORES * CORES + (CORES - 1 - lax.rem(f, CORES))])
    whole = pl.BlockSpec(memory_space=VMEM)
    return pl.pallas_call(
        partial(arrange_kernel, n_f),
        out_shape=(
            jax.ShapeDtypeStruct((n_f, here // n_t, slab), hidden.dtype),
            jax.ShapeDtypeStruct((2, here, slab), hidden.dtype),
        ),
        in_specs=[pl.BlockSpec(memory_space=SMEM)] * 2 + [pl.BlockSpec(memory_space=pl.ANY)],
        out_specs=(whole, whole),
        scratch_shapes=[DMA((n_f + 2,))],
        name="arrange",
    )(owner, place, hidden)


def head(n_f, n_t, share, block, pieces, pair, w_query, w_key, w_value, factor):
    here = pair.shape[1]
    slab = w_query.shape[0]
    n_z = n_f // CORES
    cols = w_query.shape[1] + 2 * w_key.shape[1]
    packed = here + 2 * (here // share)
    tokens = here * n_f
    whole = pl.BlockSpec(memory_space=VMEM)
    return pl.pallas_call(
        partial(head_kernel, n_f, n_t, share, block),
        out_shape=(
            jax.ShapeDtypeStruct((tokens, HD), jnp.bfloat16),
            jax.ShapeDtypeStruct((2, tokens, HD), jnp.bfloat16),
        ),
        in_specs=[whole] * 6,
        out_specs=(whole, whole),
        scratch_shapes=[
            VMEM((slab, cols), jnp.bfloat16),
            VMEM((n_f, here, slab), jnp.bfloat16),
            VMEM((n_f, CORES, n_z, packed, HD), jnp.bfloat16),
            VMEM((n_f, n_z, packed, HD), jnp.bfloat16),
            VMEM((n_f, n_z, packed, HD), jnp.bfloat16),
            VMEM((n_f, n_z, packed, HD), jnp.bfloat16),
            VMEM((packed, HD), jnp.float32),
            DMA((n_f,)),
            DMA((n_f, n_t)),
            DMA((n_f, n_t)),
            DMA((n_f,)),
            DMA((n_f,)),
            DMA((n_f, n_z)),
            DMA((n_f, n_z)),
            DMA((n_f, n_z)),
            DMA((n_f, n_z)),
            DMA((n_f, share)),
            DMA((n_f, share)),
        ],
        compiler_params=pltpu.CompilerParams(
            collective_id=0, has_side_effects=True, vmem_limit_bytes=62 * 1024 * 1024
        ),
        name="project_and_sum",
    )(pieces, pair, w_query, w_key, w_value, factor)


def attend_tile(scale, i, here, q_ref, kv_ref):
    query = q_ref[span_at(i, here), :]

    def chunk(j, state, masked):
        row_max, row_sum, accum = state
        at = span_at(j, here)
        scores = lax.dot_general(
            query, kv_ref[0, at, :], (((1,), (1,)), ((), ())), preferred_element_type=jnp.float32
        )
        if masked:
            q_pos = lax.broadcasted_iota(jnp.int32, scores.shape, 0)
            k_pos = lax.broadcasted_iota(jnp.int32, scores.shape, 1)
            scores = jnp.where(q_pos >= k_pos, scores, neg_large)
        new_max = jnp.maximum(row_max, jnp.max(scores, axis=1, keepdims=True))
        rescale = jnp.exp2((row_max - new_max) * scale)
        weights = jnp.exp2((scores - new_max) * scale)
        row_sum = row_sum * rescale + jnp.sum(weights, axis=1, keepdims=True)
        accum = accum * rescale + jnp.dot(
            weights.astype(jnp.bfloat16), kv_ref[1, at, :], preferred_element_type=jnp.float32
        )
        return (new_max, row_sum, accum)

    state = (
        jnp.full((here, 1), neg_large, jnp.float32),
        jnp.zeros((here, 1), jnp.float32),
        jnp.zeros((here, HD), jnp.float32),
    )
    state = chunk(i, state, True)
    _, row_sum, accum = lax.fori_loop(0, i, lambda j, s: chunk(j, s, False), state)
    return (accum / row_sum).astype(jnp.bfloat16)


def tail_kernel(
    n_f, n_t, block, inverse_ref, q_ref, kv_ref, w_ref, fac_ref, out_ref,
    w_scr, ctx, y, half_in, full_in, total, slabs, fin,
    line_send, line_recv, sum_send, sum_recv, slab_send, slab_recv, last_send, last_recv,
):
    f = lax.axis_index("fsdp")
    t = lax.axis_index("tp")
    n_z = n_f // CORES
    z, core = f // CORES, lax.rem(f, CORES)
    partner = z * CORES + (CORES - 1 - core)
    above, below = lax.rem(f + CORES, n_f), lax.rem(f - CORES + n_f, n_f)
    here = q_ref.shape[0] // n_f
    scale = 1.0 / (math.sqrt(HD) * math.log(2.0))
    slab = w_ref.shape[1]
    quarter = here // n_t
    per = n_f // n_t
    half = quarter // 2
    blocks = w_ref.shape[0] // block
    side = [lax.rem(t + k, n_t) for k in range(n_t)]
    along = [t + 1 - 2 * lax.rem(t, 2), lax.rem(t + n_t // 2, n_t)]
    across = n_t - 1 - t

    def order(s):
        return lax.rem(s * 3, n_f)

    def line_copy(i, zz, to, which):
        rows = span_at(i, here)
        h = lax.rem(zz + n_z, n_z) * CORES + core
        return remote(
            ctx.at[h, rows], ctx.at[h, rows], line_send.at[i, h // CORES, which],
            line_recv.at[i, h], {"fsdp": to},
        )

    def line_wait(i, h):
        rows = span_at(i, here)
        remote(
            ctx.at[h, rows], ctx.at[h, rows], line_send.at[i, 0, 0], line_recv.at[i, h],
            {"fsdp": partner},
        ).wait_recv()

    def half_copy(i, k):
        rows = slice(k * half, (k + 1) * half)
        return remote(
            y.at[i, across, rows], half_in.at[i, k], sum_send.at[i, k], sum_recv.at[i, k],
            {"tp": along[k]},
        )

    def full_copy(i, k):
        return remote(
            y.at[i, along[k]], full_in.at[i, k], sum_send.at[i, 2 + k], sum_recv.at[i, 2 + k],
            {"tp": along[k]},
        )

    def slab_copy(i):
        return remote(total.at[i], slabs.at[f], slab_send.at[i], slab_recv.at[f], {"fsdp": i})

    def last_copy(k):
        return remote(
            fin.at[side[k]], out_ref.at[span_at(t, quarter)], last_send.at[k - 1],
            last_recv.at[k - 1], {"tp": side[k]},
        )

    w_scr[...] = jnp.zeros_like(w_scr)
    scale_into(w_scr, w_ref, fac_ref, 0, blocks, block)
    greet_all(n_f, n_t, f, t)

    def relay(s, d):
        @pl.when(within(s - d, n_f))
        def _():
            i = order(s - d)

            @pl.when(z - d >= 0)
            def _():
                zz = lax.rem(z - d + n_z, n_z)
                line_wait(i, zz * CORES + core)

                @pl.when(z < n_z - 1)
                def _():
                    line_copy(i, zz, above, 1).start()

                line_copy(i, zz, partner, 0).start()

            @pl.when(z + d < n_z)
            def _():
                zz = lax.rem(z + d, n_z)
                line_wait(i, zz * CORES + core)

                @pl.when(z > 0)
                def _():
                    line_copy(i, zz, below, 2).start()

                line_copy(i, zz, partner, 0).start()

    def step(s, carry):
        @pl.when(within(s, n_f))
        def _():
            i = order(s)
            ctx[f, span_at(i, here), :] = attend_tile(scale, i, here, q_ref, kv_ref)

            @pl.when(z < n_z - 1)
            def _():
                line_copy(i, z, above, 1).start()

            @pl.when(z > 0)
            def _():
                line_copy(i, z, below, 2).start()

            line_copy(i, z, partner, 0).start()

        for d in range(1, n_z):
            relay(s, d)

        @pl.when(within(s - n_z, n_f))
        def _():
            i = order(s - n_z)
            for zz in range(n_z):
                line_wait(i, zz * CORES + (CORES - 1 - core))
            context = jnp.concatenate([ctx[h, span_at(i, here)] for h in range(n_f)], axis=1)
            part = jnp.dot(context, w_scr[...], preferred_element_type=jnp.float32).astype(
                jnp.bfloat16
            )
            for r in range(n_t):
                y[i, r] = part[r * quarter : (r + 1) * quarter, :slab]
            for k in range(2):
                half_copy(i, k).start()

        @pl.when(within(s - n_z - 1, n_f))
        def _():
            i = order(s - n_z - 1)
            for k in range(2):
                half_copy(i, k).wait_recv()
                rows = slice(k * half, (k + 1) * half)
                to = along[1 - k]
                y[i, to, rows] = (
                    y[i, to, rows].astype(jnp.float32) + half_in[i, k].astype(jnp.float32)
                ).astype(jnp.bfloat16)
                full_copy(i, 1 - k).start()

        @pl.when(within(s - n_z - 2, n_f))
        def _():
            i = order(s - n_z - 2)
            summed = y[i, t].astype(jnp.float32)
            for k in range(2):
                full_copy(i, k).wait_recv()
                summed = summed + full_in[i, k].astype(jnp.float32)
            total[i] = summed.astype(jnp.bfloat16)

            @pl.when(i == f)
            def _():
                slabs[i] = total[i]

            @pl.when(i != f)
            def _():
                slab_copy(i).start()

        @pl.when(jnp.logical_and(within(s - n_z - 3, n_f), order(s + n_f - n_z - 3) == f))
        def _():
            for d in range(1, n_f):
                source = lax.rem(f + d, n_f)
                remote(
                    total.at[0], slabs.at[source], slab_send.at[0], slab_recv.at[source],
                    {"fsdp": source},
                ).wait_recv()
            for j in range(n_f):
                fin[j // per, :, (j % per) * slab : (j % per + 1) * slab] = slabs[inverse_ref[j]]
            for k in range(1, n_t):
                last_copy(k).start()
            out_ref[span_at(t, quarter), :] = fin[t]

        return carry

    lax.fori_loop(0, n_f + n_z + 3, step, 0)

    def finish(i, carry):
        @pl.when(i != f)
        def _():
            slab_copy(i).wait_send()

        for k in range(2):
            half_copy(i, k).wait_send()
            full_copy(i, k).wait_send()
        for zz in range(n_z):
            line_copy(i, zz, partner, 0).wait_send()

            @pl.when(jnp.logical_and(zz <= z, z < n_z - 1))
            def _():
                line_copy(i, zz, above, 1).wait_send()

            @pl.when(jnp.logical_and(zz >= z, z > 0))
            def _():
                line_copy(i, zz, below, 2).wait_send()

        return carry

    lax.fori_loop(0, n_f, finish, 0)
    for k in range(1, n_t):
        source = lax.rem(t - k + n_t, n_t)
        remote(
            fin.at[0], out_ref.at[span_at(source, quarter)], last_send.at[k - 1],
            last_recv.at[k - 1], {"tp": side[1]},
        ).wait_recv()
        last_copy(k).wait_send()


def tail(n_f, n_t, block, inverse, query, kv, w_out, factor):
    tokens = query.shape[0]
    here = tokens // n_f
    quarter = here // n_t
    slab = w_out.shape[1]
    wide = slab * n_f // n_t
    n_z = n_f // CORES
    whole = pl.BlockSpec(memory_space=VMEM)
    return pl.pallas_call(
        partial(tail_kernel, n_f, n_t, block),
        out_shape=jax.ShapeDtypeStruct((here, wide), jnp.bfloat16),
        in_specs=[pl.BlockSpec(memory_space=SMEM)] + [whole] * 4,
        out_specs=whole,
        scratch_shapes=[
            VMEM((w_out.shape[0], slab + -slab % 256), jnp.bfloat16),
            VMEM((n_f, tokens, HD), jnp.bfloat16),
            VMEM((n_f, n_t, quarter, slab), jnp.bfloat16),
            VMEM((n_f, 2, quarter // 2, slab), jnp.bfloat16),
            VMEM((n_f, 2, quarter, slab), jnp.bfloat16),
            VMEM((n_f, quarter, slab), jnp.bfloat16),
            VMEM((n_f, quarter, slab), jnp.bfloat16),
            VMEM((n_t, quarter, wide), jnp.bfloat16),
            DMA((n_f, n_z, 3)),
            DMA((n_f, n_f)),
            DMA((n_f, 4)),
            DMA((n_f, 4)),
            DMA((n_f,)),
            DMA((n_f,)),
            DMA((n_t - 1,)),
            DMA((n_t - 1,)),
        ],
        compiler_params=pltpu.CompilerParams(
            collective_id=1, has_side_effects=True, vmem_limit_bytes=56 * 1024 * 1024
        ),
        name="project_out_and_sum",
    )(inverse, query, kv, w_out, factor)


def stationary_body(
    n_f, n_t, hidden, w_query, w_key, w_value, w_out, exp_query, exp_key, exp_value, exp_out, owner
):
    f = lax.axis_index("fsdp")
    t = lax.axis_index("tp")
    here, width = hidden.shape
    slab = w_query.shape[0]
    tokens = here * n_f
    block = width // exp_query.shape[0]
    slab_blocks = slab // block
    q_cols, k_cols = w_query.shape[1], w_key.shape[1]
    share = (q_cols // HD) // (k_cols // HD)
    logical = owner[f]

    def factors(exponents, cols):
        picked = lax.dynamic_slice(
            exponents, (logical * slab_blocks, t * (cols // block)), (slab_blocks, cols // block)
        )
        return jnp.repeat(jnp.exp2(picked.astype(jnp.float32)), block, axis=1)

    in_factor = jnp.concatenate(
        [factors(exp_query, q_cols), factors(exp_key, k_cols), factors(exp_value, k_cols)], axis=1
    )
    out_rows = w_out.shape[0] // block
    out_factor = jnp.repeat(
        jnp.exp2(
            lax.dynamic_slice(
                exp_out, (t * out_rows, logical * slab_blocks), (out_rows, slab_blocks)
            ).astype(jnp.float32)
        ),
        block,
        axis=1,
    )
    in_factor = jnp.pad(in_factor, ((0, -slab_blocks % 8), (0, 0)))
    out_factor = jnp.pad(out_factor, ((0, -out_rows % 8), (0, -slab % 256)))

    pieces, pair = arrange(n_f, n_t, slab, owner, hidden)
    query, kv = head(
        n_f, n_t, share, block, pieces, pair, w_query, w_key, w_value, in_factor
    )
    slab_ids = jnp.arange(n_f, dtype=jnp.int32)
    inverse = jnp.sum(
        slab_ids[:, None] * (owner[:, None] == slab_ids[None, :]).astype(jnp.int32), axis=0
    )
    return tail(n_f, n_t, block, inverse, query, kv, w_out, out_factor)


def solution(mesh):
    n_f, n_t = mesh.shape["fsdp"], mesh.shape["tp"]

    def body(*arrays):
        hidden, w_query, w_key = arrays[0], arrays[1], arrays[2]
        heads, kv_heads = w_query.shape[1] // HD, w_key.shape[1] // HD
        share = heads // kv_heads
        fits = (
            heads == n_f
            and n_t == SIDE * SIDE
            and n_f % n_t == 0
            and n_f == LINE * CORES
            and hidden.shape[0] % (16 * SIDE * n_t) == 0
            and hidden.shape[0] % (16 * share) == 0
        )
        if fits:
            return stationary_body(n_f, n_t, *arrays)
        return gather_body(*arrays)

    placed = (
        P("fsdp", None),
        P("fsdp", "tp"),
        P("fsdp", "tp"),
        P("fsdp", "tp"),
        P("tp", "fsdp"),
        P(),
        P(),
        P(),
        P(),
        P(),
    )
    return jax.shard_map(
        body, mesh=mesh, in_specs=placed, out_specs=P("fsdp", "tp"), check_vma=False
    )
```

```python
from functools import partial
import math

import jax
import jax.numpy as jnp
from jax import lax
from jax.experimental import pallas as pl
from jax.experimental.pallas import tpu as pltpu
from jax.sharding import PartitionSpec as P

HQ = 32
HK = 8
HD = 128


neg_large = -1e30


def block_factor(exponents, row_start, row_count, col_start, col_count, block_size):
    repeated = jnp.repeat(exponents, block_size, axis=0)
    picked = lax.dynamic_slice_in_dim(repeated, row_start, row_count, 0)
    repeated = jnp.repeat(picked, block_size, axis=1)
    picked = lax.dynamic_slice_in_dim(repeated, col_start, col_count, 1)
    return jnp.exp2(picked.astype(jnp.float32))


def block_update(state, query_half, pos_half, keys_part, values_part, key_pos, inv_root):
    row_max, row_sum, accum = state
    causal = pos_half[:, None] >= key_pos[None, :]
    scores = (
        jnp.einsum("tgjd,ngd->gjtn", query_half, keys_part, preferred_element_type=jnp.float32)
        * inv_root
    )
    scores = jnp.where(causal, scores, neg_large)
    new_max = jnp.maximum(row_max, jnp.max(scores, axis=3))
    rescale = jnp.exp(row_max - new_max)
    weights = jnp.where(causal, jnp.exp(scores - new_max[..., None]), 0.0)
    row_sum = row_sum * rescale + jnp.sum(weights, axis=3)
    accum = accum * rescale[..., None] + jnp.einsum(
        "gjtn,ngd->gjtd",
        weights.astype(jnp.bfloat16),
        values_part,
        preferred_element_type=jnp.float32,
    )
    return (new_max, row_sum, accum)


def keep_state(state):
    return state


def gather_body(hidden, w_query, w_key, w_value, w_out, exp_query, exp_key, exp_value, exp_out, owner):
    fsdp_index = lax.axis_index("fsdp")
    tp_index = lax.axis_index("tp")
    slab_rows = w_query.shape[0]
    groups = owner.shape[0]
    tokens = hidden.shape[0]
    model_width = hidden.shape[1]
    block_size = model_width // exp_query.shape[0]
    slab_start = owner[fsdp_index] * slab_rows
    query_cols = w_query.shape[1]
    key_cols = w_key.shape[1]

    def scaled_rows(weight, exponents):
        col_count = weight.shape[1]
        factor = block_factor(
            exponents, slab_start, slab_rows, tp_index * col_count, col_count, block_size
        )
        return (weight.astype(jnp.float32) * factor).astype(jnp.bfloat16)

    query_local = scaled_rows(w_query, exp_query)
    key_local = scaled_rows(w_key, exp_key)
    value_local = scaled_rows(w_value, exp_value)
    out_rows = w_out.shape[0]
    out_factor = block_factor(
        exp_out, tp_index * out_rows, out_rows, slab_start, slab_rows, block_size
    )
    out_local = (w_out.astype(jnp.float32) * out_factor).astype(jnp.bfloat16)
    arranged = jnp.take(hidden.reshape(tokens, groups, slab_rows), owner, axis=1).reshape(
        tokens, model_width
    )
    pieces = (
        lax.all_gather(query_local, "fsdp", axis=0, tiled=True),
        lax.all_gather(key_local, "fsdp", axis=0, tiled=True),
        lax.all_gather(value_local, "fsdp", axis=0, tiled=True),
    )
    query_sum, key_sum, value_sum = tuple(
        (jnp.dot(arranged, weight, preferred_element_type=jnp.float32) for weight in pieces)
    )
    query = query_sum.astype(jnp.bfloat16)
    key_here = key_sum.astype(jnp.bfloat16)
    value_here = value_sum.astype(jnp.bfloat16)
    half_rows = tokens // 2
    local_pos = fsdp_index * tokens + jnp.arange(tokens, dtype=jnp.int32)
    group_size = HQ // HK
    kv_heads = key_cols // HD
    query_halves = query.reshape(2, half_rows, kv_heads, group_size, HD)
    pos_halves = local_pos.reshape(2, half_rows)
    pos_top = jnp.max(pos_halves, axis=1)
    inv_root = 1.0 / math.sqrt(HD)
    one_state = (
        jnp.full((kv_heads, group_size, half_rows), neg_large, jnp.float32),
        jnp.zeros((kv_heads, group_size, half_rows), jnp.float32),
        jnp.zeros((kv_heads, group_size, half_rows, HD), jnp.float32),
    )
    offset = jnp.int32(0)
    key_piece = lax.all_gather(key_here, "fsdp", axis=0, tiled=True)
    value_piece = lax.all_gather(value_here, "fsdp", axis=0, tiled=True)
    states = list((one_state, one_state))
    piece_rows = key_piece.shape[0]
    for block_low in range(0, piece_rows, 1024):
        block_high = min(block_low + 1024, piece_rows)
        width_here = block_high - block_low
        keys_part = key_piece[block_low:block_high].reshape(width_here, kv_heads, HD)
        values_part = value_piece[block_low:block_high].reshape(width_here, kv_heads, HD)
        key_pos = offset + block_low + jnp.arange(width_here, dtype=jnp.int32)
        for attend_which in range(2):
            update = partial(
                block_update,
                query_half=query_halves[attend_which],
                pos_half=pos_halves[attend_which],
                keys_part=keys_part,
                values_part=values_part,
                key_pos=key_pos,
                inv_root=inv_root,
            )
            states[attend_which] = lax.cond(
                offset + block_low <= pos_top[attend_which],
                update,
                keep_state,
                states[attend_which],
            )
    final_states = tuple(states)
    context_parts = []
    for which in range(2):
        row_max, row_sum, accum = final_states[which]
        part_context = (accum / row_sum[..., None]).astype(jnp.bfloat16)
        context_parts.append(part_context.transpose(2, 0, 1, 3).reshape(half_rows, query_cols))
    context = jnp.concatenate(context_parts, axis=0)
    column_terms = jnp.dot(
        context,
        lax.all_gather(out_local, "fsdp", axis=1, tiled=True),
        preferred_element_type=jnp.float32,
    )
    slab_ids = jnp.arange(groups, dtype=jnp.int32)
    inverse = jnp.sum(
        slab_ids[:, None] * (owner[:, None] == slab_ids[None, :]).astype(jnp.int32), axis=0
    )
    ordered = jnp.take(column_terms.reshape(tokens, groups, slab_rows), inverse, axis=1).reshape(
        tokens, model_width
    )
    result = lax.psum_scatter(ordered.astype(jnp.bfloat16), "tp", scatter_dimension=1, tiled=True)
    return result


MESH = pl.DeviceIdType.MESH
VMEM = pltpu.VMEM
SMEM = pltpu.SMEM
DMA = pltpu.SemaphoreType.DMA
CORES = 2
LINE = 4
SIDE = 2
SPLIT = 2


def greet(peers):
    barrier = pltpu.get_barrier_semaphore()
    for device in peers:
        pl.semaphore_signal(barrier, inc=1, device_id=device, device_id_type=MESH)
    pl.semaphore_wait(barrier, len(peers))


def greet_all(n_f, n_t, f, t):
    greet(
        [{"fsdp": lax.rem(f + d, n_f)} for d in range(1, n_f)]
        + [{"tp": lax.rem(t + k, n_t)} for k in range(1, n_t)]
    )


def remote(src, dst, send, recv, device):
    return pltpu.make_async_remote_copy(
        src_ref=src,
        dst_ref=dst,
        send_sem=send,
        recv_sem=recv,
        device_id=device,
        device_id_type=MESH,
    )


def within(s, n):
    return jnp.logical_and(s >= 0, s < n)


def span_at(index, size):
    return pl.ds(pl.multiple_of(index * size, size), size)


def arrange_kernel(
    n_f, n_t, block, owner_ref, eq_hbm, ek_hbm, ev_hbm, eo_hbm, h_ref,
    pieces_ref, pair_ref, in_ref, out_ref, inverse_ref, eq_ref, ek_ref, ev_ref, eo_ref, sem, small,
):
    f = lax.axis_index("fsdp")
    t = lax.axis_index("tp")
    partner = f // CORES * CORES + (CORES - 1 - lax.rem(f, CORES))
    rows, slab = pieces_ref.shape[2], pieces_ref.shape[3]
    here = pair_ref.shape[1]

    def columns(i):
        return pl.ds(pl.multiple_of(owner_ref[i] * slab, HD), slab)

    tables = [
        pltpu.make_async_copy(source, target, small.at[k])
        for k, (source, target) in enumerate(
            ((eq_hbm, eq_ref), (ek_hbm, ek_ref), (ev_hbm, ev_ref), (eo_hbm, eo_ref))
        )
    ]
    for copy in tables:
        copy.start()
    copies = []
    for k, device in enumerate((f, partner)):
        source = h_ref.at[:, columns(device)]
        copies.append(pltpu.make_async_copy(source, pair_ref.at[k], sem.at[n_f, k]))
    for i in range(n_f):
        for p in range(SPLIT):
            start = pl.multiple_of(p * (here // SPLIT) + t * rows, rows)
            source = h_ref.at[pl.ds(start, rows), columns(i)]
            copies.append(pltpu.make_async_copy(source, pieces_ref.at[i, p], sem.at[i, p]))
    for copy in copies:
        copy.start()

    logical = owner_ref[f]
    blocks = slab // block

    def spread_out(exponents, first, width):
        shape = (exponents.shape[1], width)
        block_of = lax.broadcasted_iota(jnp.int32, shape, 1) // block + first
        chosen = lax.broadcasted_iota(jnp.int32, shape, 0) == block_of
        return jnp.dot(
            jnp.exp2(exponents.astype(jnp.float32)),
            chosen.astype(jnp.float32),
            preferred_element_type=jnp.float32,
        )

    for copy in tables:
        copy.wait()
    at = 0
    for ref in (eq_ref, ek_ref, ev_ref):
        cols = ref.shape[1] // n_t
        picked = ref[pl.ds(logical * blocks, blocks), :]
        in_ref[:blocks, at : at + cols * block] = spread_out(picked, t * cols, cols * block)
        at += cols * block
    picked = eo_ref[span_at(t, eo_ref.shape[0] // n_t), :]
    out_ref[: picked.shape[0], :] = spread_out(picked, logical * blocks, slab)
    for i in range(n_f):
        inverse_ref[owner_ref[i]] = i
    for copy in copies:
        copy.wait()


def arrange(n_f, n_t, block, owner, hidden, exponents, in_cols, out_rows, slab):
    here = hidden.shape[0]
    blocks = slab // block
    whole = pl.BlockSpec(memory_space=VMEM)
    small = pl.BlockSpec(memory_space=SMEM)
    return pl.pallas_call(
        partial(arrange_kernel, n_f, n_t, block),
        out_shape=(
            jax.ShapeDtypeStruct((n_f, SPLIT, here // (n_t * SPLIT), slab), hidden.dtype),
            jax.ShapeDtypeStruct((2, here, slab), hidden.dtype),
            jax.ShapeDtypeStruct((blocks + -blocks % 8, in_cols), jnp.float32),
            jax.ShapeDtypeStruct((out_rows // block + -(out_rows // block) % 8, slab), jnp.float32),
            jax.ShapeDtypeStruct((n_f,), jnp.int32),
        ),
        in_specs=[small] + [pl.BlockSpec(memory_space=pl.ANY)] * 5,
        out_specs=(whole, whole, whole, whole, small),
        scratch_shapes=[VMEM(e.shape, e.dtype) for e in exponents]
        + [DMA((n_f + 1, SPLIT)), DMA((len(exponents),))],
        name="arrange",
    )(owner, *exponents, hidden)


def scale_in_place(w_scr, fac_ref, block):
    for b in range(w_scr.shape[0] // block):
        rows = slice(b * block, (b + 1) * block)
        for c in range(0, fac_ref.shape[1], block):
            cols = slice(c, c + block)
            weight = w_scr[rows, cols].astype(jnp.float32)
            w_scr[rows, cols] = (weight * fac_ref[b : b + 1, cols]).astype(jnp.bfloat16)


def attend_tile(scale, i, here, q_ref, kv_ref):
    query = q_ref[span_at(i, here), :]

    def chunk(at, state, masked):
        row_max, row_sum, accum = state
        scores = lax.dot_general(
            query, kv_ref[0, at, :], (((1,), (1,)), ((), ())), preferred_element_type=jnp.float32
        )
        if masked:
            q_pos = lax.broadcasted_iota(jnp.int32, scores.shape, 0)
            k_pos = lax.broadcasted_iota(jnp.int32, scores.shape, 1)
            scores = jnp.where(q_pos >= k_pos, scores, neg_large)
        new_max = jnp.maximum(row_max, jnp.max(scores, axis=1, keepdims=True))
        rescale = jnp.exp2((row_max - new_max) * scale)
        weights = jnp.exp2((scores - new_max) * scale)
        row_sum = row_sum * rescale + jnp.sum(weights, axis=1, keepdims=True)
        accum = accum * rescale + jnp.dot(
            weights.astype(jnp.bfloat16), kv_ref[1, at, :], preferred_element_type=jnp.float32
        )
        return (new_max, row_sum, accum)

    state = (
        jnp.full((here, 1), neg_large, jnp.float32),
        jnp.zeros((here, 1), jnp.float32),
        jnp.zeros((here, HD), jnp.float32),
    )
    state = chunk(span_at(i, here), state, True)
    wide = SPAN * here
    left = lax.rem(i, SPAN)
    state = lax.fori_loop(0, left, lambda j, s: chunk(span_at(i - 1 - j, here), s, False), state)
    _, row_sum, accum = lax.fori_loop(
        0, i // SPAN, lambda j, s: chunk(span_at(j, wide), s, False), state
    )
    return (accum / row_sum).astype(jnp.bfloat16)


SPAN = 2
PROJECT = 2
PAIR = PROJECT + 1
CLOSE = PAIR + LINE - 1
ATTEND = CLOSE + 1


def layer_kernel(
    n_f, n_t, share, block, inverse_ref, pieces, pair_ref, wq_ref, wk_ref, wv_ref, wo_ref,
    fac_ref, faco_ref, out_ref,
    w_scr, wo_scr, hid, mine, px, up_in, down_in, acc, q_scr, kv_scr,
    ctx, y, half_in, full_in, total, slabs_even, slabs_odd, fin, load,
    hid_send, hid_recv, side_send, pair_send, pair_recv,
    up_send, up_recv, down_send, down_recv, kv_send, kv_recv,
    line_send, line_recv, sum_send, sum_recv, slab_send, slab_recv, last_send, last_recv,
):
    f = lax.axis_index("fsdp")
    t = lax.axis_index("tp")
    n_z = n_f // CORES
    z, core = f // CORES, lax.rem(f, CORES)
    partner = z * CORES + (CORES - 1 - core)
    above, below = lax.rem(f + CORES, n_f), lax.rem(f - CORES + n_f, n_f)
    n_b = n_f * SPLIT
    here, slab = pair_ref.shape[1] // SPLIT, pair_ref.shape[2]
    quarter = here // n_t
    part = here // share
    per = n_f // n_t
    q_cols, k_cols = wq_ref.shape[1], wk_ref.shape[1]
    scale = 1.0 / (math.sqrt(HD) * math.log(2.0))
    side = [lax.rem(t + k, n_t) for k in range(n_t)]
    along = [t + 1 - 2 * lax.rem(t, 2), lax.rem(t + n_t // 2, n_t)]
    across = n_t - 1 - t
    group, mate = f // share, lax.rem(f, share)
    slabs = (slabs_even, slabs_odd)

    def piece_copy(i, p):
        b = f * SPLIT + p
        rows = span_at(t, quarter)
        return remote(
            pieces.at[i, p], hid.at[b, rows], hid_send.at[i, p], hid_recv.at[b, t], {"fsdp": i}
        )

    def beside_copy(p):
        b = f * SPLIT + p
        rows = slice(p * here, (p + 1) * here)
        return remote(
            pair_ref.at[1, rows], hid.at[b], hid_send.at[partner, p], hid_recv.at[b, 0],
            {"fsdp": partner},
        )

    def side_copy(b, k):
        rows = span_at(t, quarter)
        return remote(
            hid.at[b, rows], hid.at[b, rows], side_send.at[b, k], hid_recv.at[b, t], {"tp": side[k]}
        )

    def pair_copy(b):
        return remote(
            mine.at[lax.rem(b, 2), CORES - 1 - core], px.at[b], pair_send.at[b], pair_recv.at[b],
            {"fsdp": partner},
        )

    def up_copy(b, zz):
        return remote(
            px.at[b, zz], up_in.at[b, zz], up_send.at[b, zz], up_recv.at[b, zz], {"fsdp": above}
        )

    def down_copy(b, zz):
        return remote(
            px.at[b, zz], down_in.at[b, zz], down_send.at[b, zz], down_recv.at[b, zz],
            {"fsdp": below},
        )

    def kv_copy(b, source, k):
        rows = pl.ds(pl.multiple_of(b * here + source * part, part), part)
        return remote(
            kv_scr.at[:, rows], kv_scr.at[:, rows], kv_send.at[b, k], kv_recv.at[b, source],
            {"fsdp": group * share + lax.rem(mate + k, share)},
        )

    def line_copy(i, zz, to, which):
        rows = span_at(i, here)
        h = lax.rem(zz + n_z, n_z) * CORES + core
        return remote(
            ctx.at[h, rows], ctx.at[h, rows], line_send.at[i, h // CORES, which],
            line_recv.at[i, h], {"fsdp": to},
        )

    def line_wait(i, h):
        rows = span_at(i, here)
        remote(
            ctx.at[h, rows], ctx.at[h, rows], line_send.at[i, 0, 0], line_recv.at[i, h],
            {"fsdp": partner},
        ).wait_recv()

    def either(i):
        first = lax.rem(i, 2)
        return along[0] + first * (along[1] - along[0]), along[1] + first * (along[0] - along[1])

    def diagonal_copy(i):
        return remote(
            y.at[i, across], half_in.at[i], sum_send.at[i, 2], sum_recv.at[i, 2],
            {"tp": either(i)[0]},
        )

    def full_copy(i, k):
        return remote(
            y.at[i, along[k]], full_in.at[i, k], sum_send.at[i, k], sum_recv.at[i, k],
            {"tp": along[k]},
        )

    def slab_copy(i, p):
        return remote(
            total.at[i], slabs[p].at[f], slab_send.at[i], slab_recv.at[f, p], {"fsdp": i // SPLIT}
        )

    def out_rows(p, source):
        return pl.ds(pl.multiple_of(p * here + source * quarter, quarter), quarter)

    def last_copy(p, k):
        return remote(
            fin.at[p, side[k]], out_ref.at[out_rows(p, t)], last_send.at[p, k - 1],
            last_recv.at[p, k - 1], {"tp": side[k]},
        )

    loads = [
        pltpu.make_async_copy(wq_ref, w_scr.at[:, :q_cols], load.at[0]),
        pltpu.make_async_copy(wk_ref, w_scr.at[:, q_cols : q_cols + k_cols], load.at[1]),
        pltpu.make_async_copy(wv_ref, w_scr.at[:, q_cols + k_cols :], load.at[2]),
        pltpu.make_async_copy(wo_ref, wo_scr.at[:, :slab], load.at[3]),
    ]
    for copy in loads:
        copy.start()
    greet_all(n_f, n_t, f, t)
    for p in range(SPLIT):
        beside_copy(p).start()
    for p in range(SPLIT):
        for d in range(n_z - 1, 0, -1):
            for c in range(CORES):

                @pl.when(z + d < n_z)
                def _():
                    piece_copy(lax.rem((z + d) * CORES + c, n_f), p).start()

                @pl.when(z - d >= 0)
                def _():
                    piece_copy(lax.rem((z - d + n_z) * CORES + c, n_f), p).start()

    for p in range(SPLIT):
        hid[f * SPLIT + p] = pair_ref[0, p * here : (p + 1) * here]
    wo_scr[:, slab:] = jnp.zeros((wo_scr.shape[0], wo_scr.shape[1] - slab), jnp.bfloat16)
    for copy in loads:
        copy.wait()
    scale_in_place(w_scr, fac_ref, block)
    scale_in_place(wo_scr, faco_ref, block)

    def piece_like(b, source):
        rows = span_at(source, quarter)
        return remote(
            pieces.at[0, 0], hid.at[b, rows], hid_send.at[0, 0], hid_recv.at[b, source],
            {"fsdp": above},
        )

    def pass_on(b):
        piece_like(b, t).wait_recv()
        for k in range(1, n_t):
            side_copy(b, k).start()

    def project(b):
        @pl.when(b // SPLIT == partner)
        def _():
            remote(
                pair_ref.at[1, :here], hid.at[b], hid_send.at[0, 0], hid_recv.at[b, 0],
                {"fsdp": partner},
            ).wait_recv()

        @pl.when(b // (SPLIT * CORES) != z)
        def _():
            for k in range(1, n_t):
                piece_like(b, side[k]).wait_recv()

        @pl.when(b >= 2)
        def _():
            pair_copy(b - 2).wait_send()

        both = jnp.dot(hid[b], w_scr[...], preferred_element_type=jnp.float32).astype(
            jnp.bfloat16
        )
        for j in range(n_f):
            g, p = j // share, j % share
            spot = mine.at[lax.rem(b, 2), j % CORES, j // CORES]
            spot[:here, :] = both[:, j * HD : (j + 1) * HD]
            rows = slice(p * part, (p + 1) * part)
            k_at = q_cols + g * HD
            v_at = q_cols + k_cols + g * HD
            spot[here : here + part, :] = both[rows, k_at : k_at + HD]
            spot[here + part :, :] = both[rows, v_at : v_at + HD]
        pair_copy(b).start()

    def join_pair(b):
        pair_copy(b).wait_recv()
        for zz in range(n_z):
            px[b, zz] = (
                px[b, zz].astype(jnp.float32) + mine[lax.rem(b, 2), core, zz].astype(jnp.float32)
            ).astype(jnp.bfloat16)

    def close(b):
        acc[...] = px[b, z].astype(jnp.float32)

        @pl.when(z > 0)
        def _():
            up_copy(b, z).wait_recv()
            acc[...] += up_in[b, z].astype(jnp.float32)

        @pl.when(z < n_z - 1)
        def _():
            down_copy(b, z).wait_recv()
            acc[...] += down_in[b, z].astype(jnp.float32)

        q_scr[span_at(b, here), :] = acc[:here, :].astype(jnp.bfloat16)
        rows = pl.ds(pl.multiple_of(b * here + mate * part, part), part)
        kv_scr[0, rows, :] = acc[here : here + part, :].astype(jnp.bfloat16)
        kv_scr[1, rows, :] = acc[here + part :, :].astype(jnp.bfloat16)
        for k in range(1, share):
            kv_copy(b, mate, k).start()

    def relay(s, d):
        @pl.when(within(s - ATTEND - d, n_b))
        def _():
            i = s - ATTEND - d

            @pl.when(z - d >= 0)
            def _():
                zz = lax.rem(z - d + n_z, n_z)
                line_wait(i, zz * CORES + core)

                @pl.when(z < n_z - 1)
                def _():
                    line_copy(i, zz, above, 1).start()

                line_copy(i, zz, partner, 0).start()

            @pl.when(z + d < n_z)
            def _():
                zz = lax.rem(z + d, n_z)
                line_wait(i, zz * CORES + core)

                @pl.when(z > 0)
                def _():
                    line_copy(i, zz, below, 2).start()

                line_copy(i, zz, partner, 0).start()

    def step(s, carry):
        @pl.when(within(s, n_b))
        def _():
            @pl.when(s // (SPLIT * CORES) != z)
            def _():
                pass_on(s)

        @pl.when(within(s - PAIR, n_b))
        def _():
            join_pair(s - PAIR)

        up_at = s - PAIR - z

        @pl.when(within(up_at, n_b))
        def _():
            b = up_at
            for zz in range(n_z - 1, 0, -1):

                @pl.when(zz > z)
                def _():
                    @pl.when(z > 0)
                    def _():
                        up_copy(b, zz).wait_recv()
                        px[b, zz] = (
                            px[b, zz].astype(jnp.float32) + up_in[b, zz].astype(jnp.float32)
                        ).astype(jnp.bfloat16)

                    up_copy(b, zz).start()

        down_at = s - PAIR - (n_z - 1 - z)

        @pl.when(within(down_at, n_b))
        def _():
            b = down_at
            for zz in range(n_z - 1):

                @pl.when(zz < z)
                def _():
                    @pl.when(z < n_z - 1)
                    def _():
                        down_copy(b, zz).wait_recv()
                        px[b, zz] = (
                            px[b, zz].astype(jnp.float32) + down_in[b, zz].astype(jnp.float32)
                        ).astype(jnp.bfloat16)

                    down_copy(b, zz).start()

        @pl.when(within(s - PROJECT, n_b))
        def _():
            project(s - PROJECT)

        @pl.when(within(s - CLOSE, n_b))
        def _():
            close(s - CLOSE)

        for d in range(1, n_z):
            relay(s, d)

        @pl.when(within(s - ATTEND, n_b))
        def _():
            i = s - ATTEND
            for k in range(1, share):
                kv_copy(i, lax.rem(mate - k + share, share), k).wait_recv()
            ctx[f, span_at(i, here), :] = attend_tile(scale, i, here, q_scr, kv_scr)

            @pl.when(z < n_z - 1)
            def _():
                line_copy(i, z, above, 1).start()

            @pl.when(z > 0)
            def _():
                line_copy(i, z, below, 2).start()

            line_copy(i, z, partner, 0).start()

        @pl.when(within(s - ATTEND - n_z, n_b))
        def _():
            i = s - ATTEND - n_z
            for zz in range(n_z):
                line_wait(i, zz * CORES + (CORES - 1 - core))
            context = jnp.concatenate([ctx[h, span_at(i, here)] for h in range(n_f)], axis=1)
            part = jnp.dot(context, wo_scr[...], preferred_element_type=jnp.float32).astype(
                jnp.bfloat16
            )
            for r in range(n_t):
                y[i, r] = part[r * quarter : (r + 1) * quarter, :slab]
            diagonal_copy(i).start()

        @pl.when(within(s - ATTEND - n_z - 1, n_b))
        def _():
            i = s - ATTEND - n_z - 1
            diagonal_copy(i).wait_recv()
            to = either(i)[1]
            y[i, to] = (y[i, to].astype(jnp.float32) + half_in[i].astype(jnp.float32)).astype(
                jnp.bfloat16
            )
            for k in range(2):
                full_copy(i, k).start()

        @pl.when(within(s - ATTEND - n_z - 2, n_b))
        def _():
            i = s - ATTEND - n_z - 2
            summed = y[i, t].astype(jnp.float32)
            for k in range(2):
                full_copy(i, k).wait_recv()
                summed = summed + full_in[i, k].astype(jnp.float32)
            total[i] = summed.astype(jnp.bfloat16)

            for p in range(SPLIT):

                @pl.when(i == f * SPLIT + p)
                def _():
                    slabs[p][f] = total[i]

                @pl.when(jnp.logical_and(i // SPLIT != f, lax.rem(i, SPLIT) == p))
                def _():
                    slab_copy(i, p).start()

        for p in range(SPLIT):

            @pl.when(s - ATTEND - n_z - 3 == f * SPLIT + p)
            def _():
                for d in range(1, n_f):
                    source = lax.rem(f + d, n_f)
                    remote(
                        total.at[0], slabs[p].at[source], slab_send.at[0], slab_recv.at[source, p],
                        {"fsdp": source},
                    ).wait_recv()
                for j in range(n_f):
                    cols = slice((j % per) * slab, (j % per + 1) * slab)
                    fin[p, j // per, :, cols] = slabs[p][inverse_ref[j]]
                for k in range(1, n_t):
                    last_copy(p, k).start()
                out_ref[out_rows(p, t), :] = fin[p, t]

        return carry

    lax.fori_loop(0, n_b + ATTEND + n_z + 3, step, 0)

    def finish_head(b, carry):
        for k in range(1, share):
            kv_copy(b, mate, k).wait_send()
        @pl.when(b >= n_b - 2)
        def _():
            pair_copy(b).wait_send()

        @pl.when(b // (SPLIT * CORES) != z)
        def _():
            piece_copy(b // SPLIT, lax.rem(b, SPLIT)).wait_send()
            for k in range(1, n_t):
                side_copy(b, k).wait_send()

        for zz in range(n_z):

            @pl.when(zz > z)
            def _():
                up_copy(b, zz).wait_send()

            @pl.when(zz < z)
            def _():
                down_copy(b, zz).wait_send()

        return carry

    lax.fori_loop(0, n_b, finish_head, 0)
    for p in range(SPLIT):
        beside_copy(p).wait_send()


    def finish(i, carry):
        @pl.when(i // SPLIT != f)
        def _():
            slab_copy(i, 0).wait_send()

        diagonal_copy(i).wait_send()
        for k in range(2):
            full_copy(i, k).wait_send()
        for zz in range(n_z):
            line_copy(i, zz, partner, 0).wait_send()

            @pl.when(jnp.logical_and(zz <= z, z < n_z - 1))
            def _():
                line_copy(i, zz, above, 1).wait_send()

            @pl.when(jnp.logical_and(zz >= z, z > 0))
            def _():
                line_copy(i, zz, below, 2).wait_send()

        return carry

    lax.fori_loop(0, n_b, finish, 0)
    for p in range(SPLIT):
        for k in range(1, n_t):
            source = lax.rem(t - k + n_t, n_t)
            remote(
                fin.at[p, 0], out_ref.at[out_rows(p, source)], last_send.at[p, k - 1],
                last_recv.at[p, k - 1], {"tp": side[1]},
            ).wait_recv()
            last_copy(p, k).wait_send()


def layer(n_f, n_t, share, block, inverse, pieces, pair, w_query, w_key, w_value, w_out, fac, faco):
    n_b = n_f * SPLIT
    here, slab = pair.shape[1] // SPLIT, pair.shape[2]
    quarter = here // n_t
    n_z = n_f // CORES
    cols = w_query.shape[1] + 2 * w_key.shape[1]
    packed = here + 2 * (here // share)
    tokens = here * n_b
    wide = slab * n_f // n_t
    whole = pl.BlockSpec(memory_space=VMEM)
    stay = pl.BlockSpec(memory_space=pl.ANY)
    small = jnp.bfloat16
    return pl.pallas_call(
        partial(layer_kernel, n_f, n_t, share, block),
        out_shape=jax.ShapeDtypeStruct((here * SPLIT, wide), small),
        in_specs=[pl.BlockSpec(memory_space=SMEM), whole, whole] + [stay] * 4 + [whole] * 2,
        out_specs=whole,
        scratch_shapes=[
            VMEM((slab, cols), small),
            VMEM((w_out.shape[0], slab + -slab % 256), small),
            VMEM((n_b, here, slab), small),
            VMEM((2, CORES, n_z, packed, HD), small),
            VMEM((n_b, n_z, packed, HD), small),
            VMEM((n_b, n_z, packed, HD), small),
            VMEM((n_b, n_z, packed, HD), small),
            VMEM((packed, HD), jnp.float32),
            VMEM((tokens, HD), small),
            VMEM((2, tokens, HD), small),
            VMEM((n_f, tokens, HD), small),
            VMEM((n_b, n_t, quarter, slab), small),
            VMEM((n_b, quarter, slab), small),
            VMEM((n_b, 2, quarter, slab), small),
            VMEM((n_b, quarter, slab), small),
            VMEM((n_f, quarter, slab), small),
            VMEM((n_f, quarter, slab), small),
            VMEM((SPLIT, n_t, quarter, wide), small),
            DMA((4,)),
            DMA((n_f, SPLIT)),
            DMA((n_b, n_t)),
            DMA((n_b, n_t)),
            DMA((n_b,)),
            DMA((n_b,)),
            DMA((n_b, n_z)),
            DMA((n_b, n_z)),
            DMA((n_b, n_z)),
            DMA((n_b, n_z)),
            DMA((n_b, share)),
            DMA((n_b, share)),
            DMA((n_b, n_z, 3)),
            DMA((n_b, n_f)),
            DMA((n_b, 3)),
            DMA((n_b, 3)),
            DMA((n_b,)),
            DMA((n_f, SPLIT)),
            DMA((SPLIT, n_t - 1)),
            DMA((SPLIT, n_t - 1)),
        ],
        compiler_params=pltpu.CompilerParams(
            collective_id=0, has_side_effects=True, vmem_limit_bytes=67043328
        ),
        name="layer",
    )(inverse, pieces, pair, w_query, w_key, w_value, w_out, fac, faco)


def stationary_body(
    n_f, n_t, hidden, w_query, w_key, w_value, w_out, exp_query, exp_key, exp_value, exp_out, owner
):
    slab = w_query.shape[0]
    block = hidden.shape[1] // exp_query.shape[0]
    q_cols, k_cols = w_query.shape[1], w_key.shape[1]
    pieces, pair, fac, faco, inverse = arrange(
        n_f, n_t, block, owner, hidden, (exp_query, exp_key, exp_value, exp_out),
        q_cols + 2 * k_cols, w_out.shape[0], slab,
    )
    return layer(
        n_f, n_t, q_cols // k_cols, block, inverse, pieces, pair, w_query, w_key, w_value, w_out,
        fac, faco,
    )


def solution(mesh):
    n_f, n_t = mesh.shape["fsdp"], mesh.shape["tp"]

    def body(*arrays):
        hidden, w_query, w_key = arrays[0], arrays[1], arrays[2]
        heads, kv_heads = w_query.shape[1] // HD, w_key.shape[1] // HD
        share = heads // kv_heads
        fits = (
            heads == n_f
            and n_t == SIDE * SIDE
            and n_f % n_t == 0
            and n_f == LINE * CORES
            and hidden.shape[0] % (16 * SPLIT * n_t) == 0
            and hidden.shape[0] % (16 * SPLIT * share) == 0
        )
        if fits:
            return stationary_body(n_f, n_t, *arrays)
        return gather_body(*arrays)

    placed = (
        P("fsdp", None),
        P("fsdp", "tp"),
        P("fsdp", "tp"),
        P("fsdp", "tp"),
        P("tp", "fsdp"),
        P(),
        P(),
        P(),
        P(),
        P(),
    )
    return jax.shard_map(
        body, mesh=mesh, in_specs=placed, out_specs=P("fsdp", "tp"), check_vma=False
    )
```

```python
from functools import partial
import math

import jax
import jax.numpy as jnp
from jax import lax
from jax.experimental import pallas as pl
from jax.experimental.pallas import tpu as pltpu
from jax.sharding import PartitionSpec as P

HQ = 32
HK = 8
HD = 128


neg_large = -1e30


def block_factor(exponents, row_start, row_count, col_start, col_count, block_size):
    repeated = jnp.repeat(exponents, block_size, axis=0)
    picked = lax.dynamic_slice_in_dim(repeated, row_start, row_count, 0)
    repeated = jnp.repeat(picked, block_size, axis=1)
    picked = lax.dynamic_slice_in_dim(repeated, col_start, col_count, 1)
    return jnp.exp2(picked.astype(jnp.float32))


def block_update(state, query_half, pos_half, keys_part, values_part, key_pos, inv_root):
    row_max, row_sum, accum = state
    causal = pos_half[:, None] >= key_pos[None, :]
    scores = (
        jnp.einsum("tgjd,ngd->gjtn", query_half, keys_part, preferred_element_type=jnp.float32)
        * inv_root
    )
    scores = jnp.where(causal, scores, neg_large)
    new_max = jnp.maximum(row_max, jnp.max(scores, axis=3))
    rescale = jnp.exp(row_max - new_max)
    weights = jnp.where(causal, jnp.exp(scores - new_max[..., None]), 0.0)
    row_sum = row_sum * rescale + jnp.sum(weights, axis=3)
    accum = accum * rescale[..., None] + jnp.einsum(
        "gjtn,ngd->gjtd",
        weights.astype(jnp.bfloat16),
        values_part,
        preferred_element_type=jnp.float32,
    )
    return (new_max, row_sum, accum)


def keep_state(state):
    return state


def gather_body(hidden, w_query, w_key, w_value, w_out, exp_query, exp_key, exp_value, exp_out, owner):
    fsdp_index = lax.axis_index("fsdp")
    tp_index = lax.axis_index("tp")
    slab_rows = w_query.shape[0]
    groups = owner.shape[0]
    tokens = hidden.shape[0]
    model_width = hidden.shape[1]
    block_size = model_width // exp_query.shape[0]
    slab_start = owner[fsdp_index] * slab_rows
    query_cols = w_query.shape[1]
    key_cols = w_key.shape[1]

    def scaled_rows(weight, exponents):
        col_count = weight.shape[1]
        factor = block_factor(
            exponents, slab_start, slab_rows, tp_index * col_count, col_count, block_size
        )
        return (weight.astype(jnp.float32) * factor).astype(jnp.bfloat16)

    query_local = scaled_rows(w_query, exp_query)
    key_local = scaled_rows(w_key, exp_key)
    value_local = scaled_rows(w_value, exp_value)
    out_rows = w_out.shape[0]
    out_factor = block_factor(
        exp_out, tp_index * out_rows, out_rows, slab_start, slab_rows, block_size
    )
    out_local = (w_out.astype(jnp.float32) * out_factor).astype(jnp.bfloat16)
    arranged = jnp.take(hidden.reshape(tokens, groups, slab_rows), owner, axis=1).reshape(
        tokens, model_width
    )
    pieces = (
        lax.all_gather(query_local, "fsdp", axis=0, tiled=True),
        lax.all_gather(key_local, "fsdp", axis=0, tiled=True),
        lax.all_gather(value_local, "fsdp", axis=0, tiled=True),
    )
    query_sum, key_sum, value_sum = tuple(
        (jnp.dot(arranged, weight, preferred_element_type=jnp.float32) for weight in pieces)
    )
    query = query_sum.astype(jnp.bfloat16)
    key_here = key_sum.astype(jnp.bfloat16)
    value_here = value_sum.astype(jnp.bfloat16)
    half_rows = tokens // 2
    local_pos = fsdp_index * tokens + jnp.arange(tokens, dtype=jnp.int32)
    group_size = HQ // HK
    kv_heads = key_cols // HD
    query_halves = query.reshape(2, half_rows, kv_heads, group_size, HD)
    pos_halves = local_pos.reshape(2, half_rows)
    pos_top = jnp.max(pos_halves, axis=1)
    inv_root = 1.0 / math.sqrt(HD)
    one_state = (
        jnp.full((kv_heads, group_size, half_rows), neg_large, jnp.float32),
        jnp.zeros((kv_heads, group_size, half_rows), jnp.float32),
        jnp.zeros((kv_heads, group_size, half_rows, HD), jnp.float32),
    )
    offset = jnp.int32(0)
    key_piece = lax.all_gather(key_here, "fsdp", axis=0, tiled=True)
    value_piece = lax.all_gather(value_here, "fsdp", axis=0, tiled=True)
    states = list((one_state, one_state))
    piece_rows = key_piece.shape[0]
    for block_low in range(0, piece_rows, 1024):
        block_high = min(block_low + 1024, piece_rows)
        width_here = block_high - block_low
        keys_part = key_piece[block_low:block_high].reshape(width_here, kv_heads, HD)
        values_part = value_piece[block_low:block_high].reshape(width_here, kv_heads, HD)
        key_pos = offset + block_low + jnp.arange(width_here, dtype=jnp.int32)
        for attend_which in range(2):
            update = partial(
                block_update,
                query_half=query_halves[attend_which],
                pos_half=pos_halves[attend_which],
                keys_part=keys_part,
                values_part=values_part,
                key_pos=key_pos,
                inv_root=inv_root,
            )
            states[attend_which] = lax.cond(
                offset + block_low <= pos_top[attend_which],
                update,
                keep_state,
                states[attend_which],
            )
    final_states = tuple(states)
    context_parts = []
    for which in range(2):
        row_max, row_sum, accum = final_states[which]
        part_context = (accum / row_sum[..., None]).astype(jnp.bfloat16)
        context_parts.append(part_context.transpose(2, 0, 1, 3).reshape(half_rows, query_cols))
    context = jnp.concatenate(context_parts, axis=0)
    column_terms = jnp.dot(
        context,
        lax.all_gather(out_local, "fsdp", axis=1, tiled=True),
        preferred_element_type=jnp.float32,
    )
    slab_ids = jnp.arange(groups, dtype=jnp.int32)
    inverse = jnp.sum(
        slab_ids[:, None] * (owner[:, None] == slab_ids[None, :]).astype(jnp.int32), axis=0
    )
    ordered = jnp.take(column_terms.reshape(tokens, groups, slab_rows), inverse, axis=1).reshape(
        tokens, model_width
    )
    result = lax.psum_scatter(ordered.astype(jnp.bfloat16), "tp", scatter_dimension=1, tiled=True)
    return result


MESH = pl.DeviceIdType.MESH
VMEM = pltpu.VMEM
SMEM = pltpu.SMEM
DMA = pltpu.SemaphoreType.DMA
CORES = 2
LINE = 4
SIDE = 2
SPLIT = 2


def greet(peers):
    barrier = pltpu.get_barrier_semaphore()
    for device in peers:
        pl.semaphore_signal(barrier, inc=1, device_id=device, device_id_type=MESH)
    pl.semaphore_wait(barrier, len(peers))


def greet_all(n_f, n_t, f, t):
    greet(
        [{"fsdp": lax.rem(f + d, n_f)} for d in range(1, n_f)]
        + [{"tp": lax.rem(t + k, n_t)} for k in range(1, n_t)]
    )


def remote(src, dst, send, recv, device):
    return pltpu.make_async_remote_copy(
        src_ref=src,
        dst_ref=dst,
        send_sem=send,
        recv_sem=recv,
        device_id=device,
        device_id_type=MESH,
    )


def within(s, n):
    return jnp.logical_and(s >= 0, s < n)


def span_at(index, size):
    return pl.ds(pl.multiple_of(index * size, size), size)


def arrange_kernel(
    n_f, n_t, block, owner_ref, eq_hbm, ek_hbm, ev_hbm, eo_hbm, h_ref,
    pieces_ref, pair_ref, in_ref, out_ref, inverse_ref, eq_ref, ek_ref, ev_ref, eo_ref, sem, small,
):
    f = lax.axis_index("fsdp")
    t = lax.axis_index("tp")
    partner = f // CORES * CORES + (CORES - 1 - lax.rem(f, CORES))
    rows, slab = pieces_ref.shape[2], pieces_ref.shape[3]
    here = pair_ref.shape[1]

    def columns(i):
        return pl.ds(pl.multiple_of(owner_ref[i] * slab, HD), slab)

    tables = [
        pltpu.make_async_copy(source, target, small.at[k])
        for k, (source, target) in enumerate(
            ((eq_hbm, eq_ref), (ek_hbm, ek_ref), (ev_hbm, ev_ref), (eo_hbm, eo_ref))
        )
    ]
    for copy in tables:
        copy.start()
    copies = []
    for k, device in enumerate((f, partner)):
        source = h_ref.at[:, columns(device)]
        copies.append(pltpu.make_async_copy(source, pair_ref.at[k], sem.at[n_f, k]))
    for i in range(n_f):
        for p in range(SPLIT):
            start = pl.multiple_of(p * (here // SPLIT) + t * rows, rows)
            source = h_ref.at[pl.ds(start, rows), columns(i)]
            copies.append(pltpu.make_async_copy(source, pieces_ref.at[i, p], sem.at[i, p]))
    for copy in copies:
        copy.start()

    logical = owner_ref[f]
    blocks = slab // block

    def spread_out(powers, first, width):
        shape = (powers.shape[1], width)
        block_of = lax.broadcasted_iota(jnp.int32, shape, 1) // block + first
        chosen = lax.broadcasted_iota(jnp.int32, shape, 0) == block_of
        return jnp.dot(
            powers,
            chosen.astype(jnp.float32),
            preferred_element_type=jnp.float32,
        )

    for copy in tables:
        copy.wait()
    at = 0
    for ref in (eq_ref, ek_ref, ev_ref):
        cols = ref.shape[0] // n_t
        shape = (in_ref.shape[0], ref.shape[1])
        row_of = lax.broadcasted_iota(jnp.int32, shape, 0) + logical * blocks
        chosen = lax.broadcasted_iota(jnp.int32, shape, 1) == row_of
        picked = lax.dot_general(
            chosen.astype(jnp.float32),
            jnp.exp2(ref[...].astype(jnp.float32)),
            (((1,), (1,)), ((), ())),
            preferred_element_type=jnp.float32,
        )
        in_ref[:, at : at + cols * block] = spread_out(picked, t * cols, cols * block)
        at += cols * block
    picked = eo_ref[span_at(t, eo_ref.shape[0] // n_t), :]
    picked = jnp.exp2(picked.astype(jnp.float32))
    out_ref[: picked.shape[0], :] = spread_out(picked, logical * blocks, slab)
    for i in range(n_f):
        inverse_ref[owner_ref[i]] = i
    for copy in copies:
        copy.wait()


def arrange(n_f, n_t, block, owner, hidden, exponents, in_cols, out_rows, slab):
    here = hidden.shape[0]
    blocks = slab // block
    whole = pl.BlockSpec(memory_space=VMEM)
    small = pl.BlockSpec(memory_space=SMEM)
    return pl.pallas_call(
        partial(arrange_kernel, n_f, n_t, block),
        out_shape=(
            jax.ShapeDtypeStruct((n_f, SPLIT, here // (n_t * SPLIT), slab), hidden.dtype),
            jax.ShapeDtypeStruct((2, here, slab), hidden.dtype),
            jax.ShapeDtypeStruct((blocks + -blocks % 8, in_cols), jnp.float32),
            jax.ShapeDtypeStruct((out_rows // block + -(out_rows // block) % 8, slab), jnp.float32),
            jax.ShapeDtypeStruct((n_f,), jnp.int32),
        ),
        in_specs=[small] + [pl.BlockSpec(memory_space=pl.ANY)] * 5,
        out_specs=(whole, whole, whole, whole, small),
        scratch_shapes=[VMEM(e.shape, e.dtype) for e in exponents]
        + [DMA((n_f + 1, SPLIT)), DMA((len(exponents),))],
        name="arrange",
    )(owner, *exponents, hidden)


def scale_in_place(w_scr, fac_ref, block):
    for b in range(w_scr.shape[0] // block):
        rows = slice(b * block, (b + 1) * block)
        for c in range(0, fac_ref.shape[1], block):
            cols = slice(c, c + block)
            weight = w_scr[rows, cols].astype(jnp.float32)
            w_scr[rows, cols] = (weight * fac_ref[b : b + 1, cols]).astype(jnp.bfloat16)


def attend_tile(scale, i, here, q_ref, kv_ref):
    query = q_ref[span_at(i, here), :]

    def chunk(at, state, masked):
        row_max, row_sum, accum = state
        scores = lax.dot_general(
            query, kv_ref[0, at, :], (((1,), (1,)), ((), ())), preferred_element_type=jnp.float32
        )
        if masked:
            q_pos = lax.broadcasted_iota(jnp.int32, scores.shape, 0)
            k_pos = lax.broadcasted_iota(jnp.int32, scores.shape, 1)
            scores = jnp.where(q_pos >= k_pos, scores, neg_large)
        new_max = jnp.maximum(row_max, jnp.max(scores, axis=1, keepdims=True))
        rescale = jnp.exp2((row_max - new_max) * scale)
        weights = jnp.exp2((scores - new_max) * scale)
        row_sum = row_sum * rescale + jnp.sum(weights, axis=1, keepdims=True)
        accum = accum * rescale + jnp.dot(
            weights.astype(jnp.bfloat16), kv_ref[1, at, :], preferred_element_type=jnp.float32
        )
        return (new_max, row_sum, accum)

    state = (
        jnp.full((here, 1), neg_large, jnp.float32),
        jnp.zeros((here, 1), jnp.float32),
        jnp.zeros((here, HD), jnp.float32),
    )
    state = chunk(span_at(i, here), state, True)
    wide = SPAN * here
    left = lax.rem(i, SPAN)
    state = lax.fori_loop(0, left, lambda j, s: chunk(span_at(i - 1 - j, here), s, False), state)
    _, row_sum, accum = lax.fori_loop(
        0, i // SPAN, lambda j, s: chunk(span_at(j, wide), s, False), state
    )
    return (accum / row_sum).astype(jnp.bfloat16)


SPAN = 4
PROJECT = 2
PAIR = PROJECT + 1
CLOSE = PAIR + LINE - 1
ATTEND = CLOSE + 1


def layer_kernel(
    n_f, n_t, share, block, inverse_ref, pieces, pair_ref, wq_ref, wk_ref, wv_ref, wo_ref,
    fac_ref, faco_ref, out_ref,
    w_scr, wo_scr, hid, mine, px, up_in, down_in, acc, q_scr, kv_scr,
    ctx, y, half_in, full_in, total, slabs_even, slabs_odd, fin, load,
    hid_send, hid_recv, side_send, pair_send, pair_recv,
    up_send, up_recv, down_send, down_recv, kv_send, kv_recv,
    line_send, line_recv, sum_send, sum_recv, slab_send, slab_recv, last_send, last_recv,
):
    f = lax.axis_index("fsdp")
    t = lax.axis_index("tp")
    n_z = n_f // CORES
    z, core = f // CORES, lax.rem(f, CORES)
    partner = z * CORES + (CORES - 1 - core)
    above, below = lax.rem(f + CORES, n_f), lax.rem(f - CORES + n_f, n_f)
    n_b = n_f * SPLIT
    here, slab = pair_ref.shape[1] // SPLIT, pair_ref.shape[2]
    quarter = here // n_t
    part = here // share
    per = n_f // n_t
    q_cols, k_cols = wq_ref.shape[1], wk_ref.shape[1]
    scale = 1.0 / (math.sqrt(HD) * math.log(2.0))
    side = [lax.rem(t + k, n_t) for k in range(n_t)]
    along = [t + 1 - 2 * lax.rem(t, 2), lax.rem(t + n_t // 2, n_t)]
    across = n_t - 1 - t
    group, mate = f // share, lax.rem(f, share)
    slabs = (slabs_even, slabs_odd)

    def piece_copy(i, p):
        b = f * SPLIT + p
        rows = span_at(t, quarter)
        return remote(
            pieces.at[i, p], hid.at[b, rows], hid_send.at[i, p], hid_recv.at[b, t], {"fsdp": i}
        )

    def beside_copy(p):
        b = f * SPLIT + p
        rows = slice(p * here, (p + 1) * here)
        return remote(
            pair_ref.at[1, rows], hid.at[b], hid_send.at[partner, p], hid_recv.at[b, 0],
            {"fsdp": partner},
        )

    def side_copy(b, k):
        rows = span_at(t, quarter)
        return remote(
            hid.at[b, rows], hid.at[b, rows], side_send.at[b, k], hid_recv.at[b, t], {"tp": side[k]}
        )

    def pair_copy(b):
        return remote(
            mine.at[lax.rem(b, 2), CORES - 1 - core], px.at[b], pair_send.at[b], pair_recv.at[b],
            {"fsdp": partner},
        )

    def up_copy(b, zz):
        return remote(
            px.at[b, zz], up_in.at[b, zz], up_send.at[b, zz], up_recv.at[b, zz], {"fsdp": above}
        )

    def down_copy(b, zz):
        return remote(
            px.at[b, zz], down_in.at[b, zz], down_send.at[b, zz], down_recv.at[b, zz],
            {"fsdp": below},
        )

    def kv_copy(b, source, k):
        rows = pl.ds(pl.multiple_of(b * here + source * part, part), part)
        return remote(
            kv_scr.at[:, rows], kv_scr.at[:, rows], kv_send.at[b, k], kv_recv.at[b, source],
            {"fsdp": group * share + lax.rem(mate + k, share)},
        )

    def line_copy(i, zz, to, which):
        rows = span_at(i, here)
        h = lax.rem(zz + n_z, n_z) * CORES + core
        return remote(
            ctx.at[h, rows], ctx.at[h, rows], line_send.at[i, h // CORES, which],
            line_recv.at[i, h], {"fsdp": to},
        )

    def line_wait(i, h):
        rows = span_at(i, here)
        remote(
            ctx.at[h, rows], ctx.at[h, rows], line_send.at[i, 0, 0], line_recv.at[i, h],
            {"fsdp": partner},
        ).wait_recv()

    def either(i):
        first = lax.rem(i, 2)
        return along[0] + first * (along[1] - along[0]), along[1] + first * (along[0] - along[1])

    def diagonal_copy(i):
        return remote(
            y.at[i, across], half_in.at[i], sum_send.at[i, 2], sum_recv.at[i, 2],
            {"tp": either(i)[0]},
        )

    def full_copy(i, k):
        return remote(
            y.at[i, along[k]], full_in.at[i, k], sum_send.at[i, k], sum_recv.at[i, k],
            {"tp": along[k]},
        )

    def slab_copy(i, p):
        return remote(
            total.at[i], slabs[p].at[f], slab_send.at[i], slab_recv.at[f, p], {"fsdp": i // SPLIT}
        )

    def out_rows(p, source):
        return pl.ds(pl.multiple_of(p * here + source * quarter, quarter), quarter)

    def last_copy(p, k):
        return remote(
            fin.at[p, side[k]], out_ref.at[out_rows(p, t)], last_send.at[p, k - 1],
            last_recv.at[p, k - 1], {"tp": side[k]},
        )

    loads = [
        pltpu.make_async_copy(wq_ref, w_scr.at[:, :q_cols], load.at[0]),
        pltpu.make_async_copy(wk_ref, w_scr.at[:, q_cols : q_cols + k_cols], load.at[1]),
        pltpu.make_async_copy(wv_ref, w_scr.at[:, q_cols + k_cols :], load.at[2]),
        pltpu.make_async_copy(wo_ref, wo_scr.at[:, :slab], load.at[3]),
    ]
    for copy in loads:
        copy.start()
    greet_all(n_f, n_t, f, t)
    for p in range(SPLIT):
        beside_copy(p).start()
    for p in range(SPLIT):
        for d in range(n_z - 1, 0, -1):
            for c in range(CORES):

                @pl.when(z + d < n_z)
                def _():
                    piece_copy(lax.rem((z + d) * CORES + c, n_f), p).start()

                @pl.when(z - d >= 0)
                def _():
                    piece_copy(lax.rem((z - d + n_z) * CORES + c, n_f), p).start()

    for p in range(SPLIT):
        hid[f * SPLIT + p] = pair_ref[0, p * here : (p + 1) * here]
    wo_scr[:, slab:] = jnp.zeros((wo_scr.shape[0], wo_scr.shape[1] - slab), jnp.bfloat16)
    for copy in loads:
        copy.wait()
    scale_in_place(w_scr, fac_ref, block)
    scale_in_place(wo_scr, faco_ref, block)

    def piece_like(b, source):
        rows = span_at(source, quarter)
        return remote(
            pieces.at[0, 0], hid.at[b, rows], hid_send.at[0, 0], hid_recv.at[b, source],
            {"fsdp": above},
        )

    def pass_on(b):
        piece_like(b, t).wait_recv()
        for k in range(1, n_t):
            side_copy(b, k).start()

    def project(b):
        @pl.when(b // SPLIT == partner)
        def _():
            remote(
                pair_ref.at[1, :here], hid.at[b], hid_send.at[0, 0], hid_recv.at[b, 0],
                {"fsdp": partner},
            ).wait_recv()

        @pl.when(b // (SPLIT * CORES) != z)
        def _():
            for k in range(1, n_t):
                piece_like(b, side[k]).wait_recv()

        @pl.when(b >= 2)
        def _():
            pair_copy(b - 2).wait_send()

        both = jnp.dot(hid[b], w_scr[...], preferred_element_type=jnp.float32).astype(
            jnp.bfloat16
        )
        for j in range(n_f):
            g, p = j // share, j % share
            spot = mine.at[lax.rem(b, 2), j % CORES, j // CORES]
            spot[:here, :] = both[:, j * HD : (j + 1) * HD]
            rows = slice(p * part, (p + 1) * part)
            k_at = q_cols + g * HD
            v_at = q_cols + k_cols + g * HD
            spot[here : here + part, :] = both[rows, k_at : k_at + HD]
            spot[here + part :, :] = both[rows, v_at : v_at + HD]
        pair_copy(b).start()

    def join_pair(b):
        pair_copy(b).wait_recv()
        for zz in range(n_z):
            px[b, zz] = (
                px[b, zz].astype(jnp.float32) + mine[lax.rem(b, 2), core, zz].astype(jnp.float32)
            ).astype(jnp.bfloat16)

    def close(b):
        acc[...] = px[b, z].astype(jnp.float32)

        @pl.when(z > 0)
        def _():
            up_copy(b, z).wait_recv()
            acc[...] += up_in[b, z].astype(jnp.float32)

        @pl.when(z < n_z - 1)
        def _():
            down_copy(b, z).wait_recv()
            acc[...] += down_in[b, z].astype(jnp.float32)

        q_scr[span_at(b, here), :] = acc[:here, :].astype(jnp.bfloat16)
        rows = pl.ds(pl.multiple_of(b * here + mate * part, part), part)
        kv_scr[0, rows, :] = acc[here : here + part, :].astype(jnp.bfloat16)
        kv_scr[1, rows, :] = acc[here + part :, :].astype(jnp.bfloat16)
        for k in range(1, share):
            kv_copy(b, mate, k).start()

    def relay(s, d):
        @pl.when(within(s - ATTEND - d, n_b))
        def _():
            i = s - ATTEND - d

            @pl.when(z - d >= 0)
            def _():
                zz = lax.rem(z - d + n_z, n_z)
                line_wait(i, zz * CORES + core)

                @pl.when(z < n_z - 1)
                def _():
                    line_copy(i, zz, above, 1).start()

                line_copy(i, zz, partner, 0).start()

            @pl.when(z + d < n_z)
            def _():
                zz = lax.rem(z + d, n_z)
                line_wait(i, zz * CORES + core)

                @pl.when(z > 0)
                def _():
                    line_copy(i, zz, below, 2).start()

                line_copy(i, zz, partner, 0).start()

    def step(s, carry):
        @pl.when(within(s, n_b))
        def _():
            @pl.when(s // (SPLIT * CORES) != z)
            def _():
                pass_on(s)

        @pl.when(within(s - PAIR, n_b))
        def _():
            join_pair(s - PAIR)

        up_at = s - PAIR - z

        @pl.when(within(up_at, n_b))
        def _():
            b = up_at
            for zz in range(n_z - 1, 0, -1):

                @pl.when(zz > z)
                def _():
                    @pl.when(z > 0)
                    def _():
                        up_copy(b, zz).wait_recv()
                        px[b, zz] = (
                            px[b, zz].astype(jnp.float32) + up_in[b, zz].astype(jnp.float32)
                        ).astype(jnp.bfloat16)

                    up_copy(b, zz).start()

        down_at = s - PAIR - (n_z - 1 - z)

        @pl.when(within(down_at, n_b))
        def _():
            b = down_at
            for zz in range(n_z - 1):

                @pl.when(zz < z)
                def _():
                    @pl.when(z < n_z - 1)
                    def _():
                        down_copy(b, zz).wait_recv()
                        px[b, zz] = (
                            px[b, zz].astype(jnp.float32) + down_in[b, zz].astype(jnp.float32)
                        ).astype(jnp.bfloat16)

                    down_copy(b, zz).start()

        @pl.when(within(s - PROJECT, n_b))
        def _():
            project(s - PROJECT)

        @pl.when(within(s - CLOSE, n_b))
        def _():
            close(s - CLOSE)

        @pl.when(within(s - ATTEND, n_b))
        def _():
            i = s - ATTEND
            for k in range(1, share):
                kv_copy(i, lax.rem(mate - k + share, share), k).wait_recv()
            ctx[f, span_at(i, here), :] = attend_tile(scale, i, here, q_scr, kv_scr)

            @pl.when(z < n_z - 1)
            def _():
                line_copy(i, z, above, 1).start()

            @pl.when(z > 0)
            def _():
                line_copy(i, z, below, 2).start()

            line_copy(i, z, partner, 0).start()

        for d in range(1, n_z):
            relay(s, d)

        @pl.when(within(s - ATTEND - n_z, n_b))
        def _():
            i = s - ATTEND - n_z
            for zz in range(n_z):
                line_wait(i, zz * CORES + (CORES - 1 - core))
            context = jnp.concatenate([ctx[h, span_at(i, here)] for h in range(n_f)], axis=1)
            part = jnp.dot(context, wo_scr[...], preferred_element_type=jnp.float32).astype(
                jnp.bfloat16
            )
            for r in range(n_t):
                y[i, r] = part[r * quarter : (r + 1) * quarter, :slab]
            diagonal_copy(i).start()

        @pl.when(within(s - ATTEND - n_z - 1, n_b))
        def _():
            i = s - ATTEND - n_z - 1
            diagonal_copy(i).wait_recv()
            to = either(i)[1]
            y[i, to] = (y[i, to].astype(jnp.float32) + half_in[i].astype(jnp.float32)).astype(
                jnp.bfloat16
            )
            for k in range(2):
                full_copy(i, k).start()

        @pl.when(within(s - ATTEND - n_z - 2, n_b))
        def _():
            i = s - ATTEND - n_z - 2
            summed = y[i, t].astype(jnp.float32)
            for k in range(2):
                full_copy(i, k).wait_recv()
                summed = summed + full_in[i, k].astype(jnp.float32)
            total[i] = summed.astype(jnp.bfloat16)

            for p in range(SPLIT):

                @pl.when(i == f * SPLIT + p)
                def _():
                    slabs[p][f] = total[i]

                @pl.when(jnp.logical_and(i // SPLIT != f, lax.rem(i, SPLIT) == p))
                def _():
                    slab_copy(i, p).start()

        for p in range(SPLIT):

            @pl.when(s - ATTEND - n_z - 3 == f * SPLIT + p)
            def _():
                for d in range(1, n_f):
                    source = lax.rem(f + d, n_f)
                    remote(
                        total.at[0], slabs[p].at[source], slab_send.at[0], slab_recv.at[source, p],
                        {"fsdp": source},
                    ).wait_recv()
                for j in range(n_f):
                    cols = slice((j % per) * slab, (j % per + 1) * slab)
                    fin[p, j // per, :, cols] = slabs[p][inverse_ref[j]]
                for k in range(1, n_t):
                    last_copy(p, k).start()
                out_ref[out_rows(p, t), :] = fin[p, t]

        return carry

    lax.fori_loop(0, n_b + ATTEND + n_z + 3, step, 0)

    def finish_head(b, carry):
        for k in range(1, share):
            kv_copy(b, mate, k).wait_send()
        @pl.when(b >= n_b - 2)
        def _():
            pair_copy(b).wait_send()

        @pl.when(b // (SPLIT * CORES) != z)
        def _():
            piece_copy(b // SPLIT, lax.rem(b, SPLIT)).wait_send()
            for k in range(1, n_t):
                side_copy(b, k).wait_send()

        for zz in range(n_z):

            @pl.when(zz > z)
            def _():
                up_copy(b, zz).wait_send()

            @pl.when(zz < z)
            def _():
                down_copy(b, zz).wait_send()

        return carry

    lax.fori_loop(0, n_b, finish_head, 0)
    for p in range(SPLIT):
        beside_copy(p).wait_send()


    def finish(i, carry):
        @pl.when(i // SPLIT != f)
        def _():
            slab_copy(i, 0).wait_send()

        diagonal_copy(i).wait_send()
        for k in range(2):
            full_copy(i, k).wait_send()
        for zz in range(n_z):
            line_copy(i, zz, partner, 0).wait_send()

            @pl.when(jnp.logical_and(zz <= z, z < n_z - 1))
            def _():
                line_copy(i, zz, above, 1).wait_send()

            @pl.when(jnp.logical_and(zz >= z, z > 0))
            def _():
                line_copy(i, zz, below, 2).wait_send()

        return carry

    lax.fori_loop(0, n_b, finish, 0)
    for p in range(SPLIT):
        for k in range(1, n_t):
            source = lax.rem(t - k + n_t, n_t)
            remote(
                fin.at[p, 0], out_ref.at[out_rows(p, source)], last_send.at[p, k - 1],
                last_recv.at[p, k - 1], {"tp": side[1]},
            ).wait_recv()
            last_copy(p, k).wait_send()


def layer(n_f, n_t, share, block, inverse, pieces, pair, w_query, w_key, w_value, w_out, fac, faco):
    n_b = n_f * SPLIT
    here, slab = pair.shape[1] // SPLIT, pair.shape[2]
    quarter = here // n_t
    n_z = n_f // CORES
    cols = w_query.shape[1] + 2 * w_key.shape[1]
    packed = here + 2 * (here // share)
    tokens = here * n_b
    wide = slab * n_f // n_t
    whole = pl.BlockSpec(memory_space=VMEM)
    stay = pl.BlockSpec(memory_space=pl.ANY)
    small = jnp.bfloat16
    return pl.pallas_call(
        partial(layer_kernel, n_f, n_t, share, block),
        out_shape=jax.ShapeDtypeStruct((here * SPLIT, wide), small),
        in_specs=[pl.BlockSpec(memory_space=SMEM), whole, whole] + [stay] * 4 + [whole] * 2,
        out_specs=whole,
        scratch_shapes=[
            VMEM((slab, cols), small),
            VMEM((w_out.shape[0], slab + -slab % 256), small),
            VMEM((n_b, here, slab), small),
            VMEM((2, CORES, n_z, packed, HD), small),
            VMEM((n_b, n_z, packed, HD), small),
            VMEM((n_b, n_z, packed, HD), small),
            VMEM((n_b, n_z, packed, HD), small),
            VMEM((packed, HD), jnp.float32),
            VMEM((tokens, HD), small),
            VMEM((2, tokens, HD), small),
            VMEM((n_f, tokens, HD), small),
            VMEM((n_b, n_t, quarter, slab), small),
            VMEM((n_b, quarter, slab), small),
            VMEM((n_b, 2, quarter, slab), small),
            VMEM((n_b, quarter, slab), small),
            VMEM((n_f, quarter, slab), small),
            VMEM((n_f, quarter, slab), small),
            VMEM((SPLIT, n_t, quarter, wide), small),
            DMA((4,)),
            DMA((n_f, SPLIT)),
            DMA((n_b, n_t)),
            DMA((n_b, n_t)),
            DMA((n_b,)),
            DMA((n_b,)),
            DMA((n_b, n_z)),
            DMA((n_b, n_z)),
            DMA((n_b, n_z)),
            DMA((n_b, n_z)),
            DMA((n_b, share)),
            DMA((n_b, share)),
            DMA((n_b, n_z, 3)),
            DMA((n_b, n_f)),
            DMA((n_b, 3)),
            DMA((n_b, 3)),
            DMA((n_b,)),
            DMA((n_f, SPLIT)),
            DMA((SPLIT, n_t - 1)),
            DMA((SPLIT, n_t - 1)),
        ],
        compiler_params=pltpu.CompilerParams(
            collective_id=0, has_side_effects=True, vmem_limit_bytes=67043328
        ),
        name="layer",
    )(inverse, pieces, pair, w_query, w_key, w_value, w_out, fac, faco)


def stationary_body(
    n_f, n_t, hidden, w_query, w_key, w_value, w_out, exp_query, exp_key, exp_value, exp_out, owner
):
    slab = w_query.shape[0]
    block = hidden.shape[1] // exp_query.shape[0]
    q_cols, k_cols = w_query.shape[1], w_key.shape[1]
    pieces, pair, fac, faco, inverse = arrange(
        n_f, n_t, block, owner, hidden, (exp_query.T, exp_key.T, exp_value.T, exp_out),
        q_cols + 2 * k_cols, w_out.shape[0], slab,
    )
    return layer(
        n_f, n_t, q_cols // k_cols, block, inverse, pieces, pair, w_query, w_key, w_value, w_out,
        fac, faco,
    )


def solution(mesh):
    n_f, n_t = mesh.shape["fsdp"], mesh.shape["tp"]

    def body(*arrays):
        hidden, w_query, w_key = arrays[0], arrays[1], arrays[2]
        heads, kv_heads = w_query.shape[1] // HD, w_key.shape[1] // HD
        share = heads // kv_heads
        fits = (
            heads == n_f
            and n_t == SIDE * SIDE
            and n_f % n_t == 0
            and n_f == LINE * CORES
            and hidden.shape[0] % (16 * SPLIT * n_t) == 0
            and hidden.shape[0] % (16 * SPLIT * share) == 0
        )
        if fits:
            return stationary_body(n_f, n_t, *arrays)
        return gather_body(*arrays)

    placed = (
        P("fsdp", None),
        P("fsdp", "tp"),
        P("fsdp", "tp"),
        P("fsdp", "tp"),
        P("tp", "fsdp"),
        P(),
        P(),
        P(),
        P(),
        P(),
    )
    return jax.shard_map(
        body, mesh=mesh, in_specs=placed, out_specs=P("fsdp", "tp"), check_vma=False
    )
```

```python
from functools import partial
import math

import jax
import jax.numpy as jnp
from jax import lax
from jax.experimental import pallas as pl
from jax.experimental.pallas import tpu as pltpu
from jax.sharding import PartitionSpec as P

HQ = 32
HK = 8
HD = 128


neg_large = -1e30


def block_factor(exponents, row_start, row_count, col_start, col_count, block_size):
    repeated = jnp.repeat(exponents, block_size, axis=0)
    picked = lax.dynamic_slice_in_dim(repeated, row_start, row_count, 0)
    repeated = jnp.repeat(picked, block_size, axis=1)
    picked = lax.dynamic_slice_in_dim(repeated, col_start, col_count, 1)
    return jnp.exp2(picked.astype(jnp.float32))


def block_update(state, query_half, pos_half, keys_part, values_part, key_pos, inv_root):
    row_max, row_sum, accum = state
    causal = pos_half[:, None] >= key_pos[None, :]
    scores = (
        jnp.einsum("tgjd,ngd->gjtn", query_half, keys_part, preferred_element_type=jnp.float32)
        * inv_root
    )
    scores = jnp.where(causal, scores, neg_large)
    new_max = jnp.maximum(row_max, jnp.max(scores, axis=3))
    rescale = jnp.exp(row_max - new_max)
    weights = jnp.where(causal, jnp.exp(scores - new_max[..., None]), 0.0)
    row_sum = row_sum * rescale + jnp.sum(weights, axis=3)
    accum = accum * rescale[..., None] + jnp.einsum(
        "gjtn,ngd->gjtd",
        weights.astype(jnp.bfloat16),
        values_part,
        preferred_element_type=jnp.float32,
    )
    return (new_max, row_sum, accum)


def keep_state(state):
    return state


def gather_body(hidden, w_query, w_key, w_value, w_out, exp_query, exp_key, exp_value, exp_out, owner):
    fsdp_index = lax.axis_index("fsdp")
    tp_index = lax.axis_index("tp")
    slab_rows = w_query.shape[0]
    groups = owner.shape[0]
    tokens = hidden.shape[0]
    model_width = hidden.shape[1]
    block_size = model_width // exp_query.shape[0]
    slab_start = owner[fsdp_index] * slab_rows
    query_cols = w_query.shape[1]
    key_cols = w_key.shape[1]

    def scaled_rows(weight, exponents):
        col_count = weight.shape[1]
        factor = block_factor(
            exponents, slab_start, slab_rows, tp_index * col_count, col_count, block_size
        )
        return (weight.astype(jnp.float32) * factor).astype(jnp.bfloat16)

    query_local = scaled_rows(w_query, exp_query)
    key_local = scaled_rows(w_key, exp_key)
    value_local = scaled_rows(w_value, exp_value)
    out_rows = w_out.shape[0]
    out_factor = block_factor(
        exp_out, tp_index * out_rows, out_rows, slab_start, slab_rows, block_size
    )
    out_local = (w_out.astype(jnp.float32) * out_factor).astype(jnp.bfloat16)
    arranged = jnp.take(hidden.reshape(tokens, groups, slab_rows), owner, axis=1).reshape(
        tokens, model_width
    )
    pieces = (
        lax.all_gather(query_local, "fsdp", axis=0, tiled=True),
        lax.all_gather(key_local, "fsdp", axis=0, tiled=True),
        lax.all_gather(value_local, "fsdp", axis=0, tiled=True),
    )
    query_sum, key_sum, value_sum = tuple(
        (jnp.dot(arranged, weight, preferred_element_type=jnp.float32) for weight in pieces)
    )
    query = query_sum.astype(jnp.bfloat16)
    key_here = key_sum.astype(jnp.bfloat16)
    value_here = value_sum.astype(jnp.bfloat16)
    half_rows = tokens // 2
    local_pos = fsdp_index * tokens + jnp.arange(tokens, dtype=jnp.int32)
    group_size = HQ // HK
    kv_heads = key_cols // HD
    query_halves = query.reshape(2, half_rows, kv_heads, group_size, HD)
    pos_halves = local_pos.reshape(2, half_rows)
    pos_top = jnp.max(pos_halves, axis=1)
    inv_root = 1.0 / math.sqrt(HD)
    one_state = (
        jnp.full((kv_heads, group_size, half_rows), neg_large, jnp.float32),
        jnp.zeros((kv_heads, group_size, half_rows), jnp.float32),
        jnp.zeros((kv_heads, group_size, half_rows, HD), jnp.float32),
    )
    offset = jnp.int32(0)
    key_piece = lax.all_gather(key_here, "fsdp", axis=0, tiled=True)
    value_piece = lax.all_gather(value_here, "fsdp", axis=0, tiled=True)
    states = list((one_state, one_state))
    piece_rows = key_piece.shape[0]
    for block_low in range(0, piece_rows, 1024):
        block_high = min(block_low + 1024, piece_rows)
        width_here = block_high - block_low
        keys_part = key_piece[block_low:block_high].reshape(width_here, kv_heads, HD)
        values_part = value_piece[block_low:block_high].reshape(width_here, kv_heads, HD)
        key_pos = offset + block_low + jnp.arange(width_here, dtype=jnp.int32)
        for attend_which in range(2):
            update = partial(
                block_update,
                query_half=query_halves[attend_which],
                pos_half=pos_halves[attend_which],
                keys_part=keys_part,
                values_part=values_part,
                key_pos=key_pos,
                inv_root=inv_root,
            )
            states[attend_which] = lax.cond(
                offset + block_low <= pos_top[attend_which],
                update,
                keep_state,
                states[attend_which],
            )
    final_states = tuple(states)
    context_parts = []
    for which in range(2):
        row_max, row_sum, accum = final_states[which]
        part_context = (accum / row_sum[..., None]).astype(jnp.bfloat16)
        context_parts.append(part_context.transpose(2, 0, 1, 3).reshape(half_rows, query_cols))
    context = jnp.concatenate(context_parts, axis=0)
    column_terms = jnp.dot(
        context,
        lax.all_gather(out_local, "fsdp", axis=1, tiled=True),
        preferred_element_type=jnp.float32,
    )
    slab_ids = jnp.arange(groups, dtype=jnp.int32)
    inverse = jnp.sum(
        slab_ids[:, None] * (owner[:, None] == slab_ids[None, :]).astype(jnp.int32), axis=0
    )
    ordered = jnp.take(column_terms.reshape(tokens, groups, slab_rows), inverse, axis=1).reshape(
        tokens, model_width
    )
    result = lax.psum_scatter(ordered.astype(jnp.bfloat16), "tp", scatter_dimension=1, tiled=True)
    return result


MESH = pl.DeviceIdType.MESH
VMEM = pltpu.VMEM
SMEM = pltpu.SMEM
DMA = pltpu.SemaphoreType.DMA
CORES = 2
LINE = 4
SIDE = 2
SPLIT = 2


def greet(peers):
    barrier = pltpu.get_barrier_semaphore()
    for device in peers:
        pl.semaphore_signal(barrier, inc=1, device_id=device, device_id_type=MESH)
    pl.semaphore_wait(barrier, len(peers))


def greet_all(n_f, n_t, f, t):
    greet(
        [{"fsdp": lax.rem(f + d, n_f)} for d in range(1, n_f)]
        + [{"tp": lax.rem(t + k, n_t)} for k in range(1, n_t)]
    )


def remote(src, dst, send, recv, device):
    return pltpu.make_async_remote_copy(
        src_ref=src,
        dst_ref=dst,
        send_sem=send,
        recv_sem=recv,
        device_id=device,
        device_id_type=MESH,
    )


def within(s, n):
    return jnp.logical_and(s >= 0, s < n)


def span_at(index, size):
    return pl.ds(pl.multiple_of(index * size, size), size)


def arrange_kernel(
    n_f, n_t, block, owner_ref, eq_hbm, ek_hbm, ev_hbm, eo_hbm, h_ref,
    pieces_ref, pair_ref, in_ref, out_ref, inverse_ref, eq_ref, ek_ref, ev_ref, eo_ref, sem, small,
):
    f = lax.axis_index("fsdp")
    t = lax.axis_index("tp")
    partner = f // CORES * CORES + (CORES - 1 - lax.rem(f, CORES))
    rows, slab = pieces_ref.shape[2], pieces_ref.shape[3]
    here = pair_ref.shape[1]

    def columns(i):
        return pl.ds(pl.multiple_of(owner_ref[i] * slab, HD), slab)

    tables = [
        pltpu.make_async_copy(source, target, small.at[k])
        for k, (source, target) in enumerate(
            ((eq_hbm, eq_ref), (ek_hbm, ek_ref), (ev_hbm, ev_ref), (eo_hbm, eo_ref))
        )
    ]
    for copy in tables:
        copy.start()
    copies = []
    for k, device in enumerate((f, partner)):
        source = h_ref.at[:, columns(device)]
        copies.append(pltpu.make_async_copy(source, pair_ref.at[k], sem.at[n_f, k]))
    for i in range(n_f):
        for p in range(SPLIT):
            start = pl.multiple_of(p * (here // SPLIT) + t * rows, rows)
            source = h_ref.at[pl.ds(start, rows), columns(i)]
            copies.append(pltpu.make_async_copy(source, pieces_ref.at[i, p], sem.at[i, p]))
    for copy in copies:
        copy.start()

    logical = owner_ref[f]
    blocks = slab // block

    def spread_out(powers, first, width):
        shape = (powers.shape[1], width)
        block_of = lax.broadcasted_iota(jnp.int32, shape, 1) // block + first
        chosen = lax.broadcasted_iota(jnp.int32, shape, 0) == block_of
        return jnp.dot(
            powers,
            chosen.astype(jnp.float32),
            preferred_element_type=jnp.float32,
        )

    for copy in tables:
        copy.wait()
    at = 0
    for ref in (eq_ref, ek_ref, ev_ref):
        cols = ref.shape[0] // n_t
        shape = (in_ref.shape[0], ref.shape[1])
        row_of = lax.broadcasted_iota(jnp.int32, shape, 0) + logical * blocks
        chosen = lax.broadcasted_iota(jnp.int32, shape, 1) == row_of
        picked = lax.dot_general(
            chosen.astype(jnp.float32),
            jnp.exp2(ref[...].astype(jnp.float32)),
            (((1,), (1,)), ((), ())),
            preferred_element_type=jnp.float32,
        )
        in_ref[:, at : at + cols * block] = spread_out(picked, t * cols, cols * block)
        at += cols * block
    picked = eo_ref[span_at(t, eo_ref.shape[0] // n_t), :]
    picked = jnp.exp2(picked.astype(jnp.float32))
    out_ref[: picked.shape[0], :] = spread_out(picked, logical * blocks, slab)
    for i in range(n_f):
        inverse_ref[owner_ref[i]] = i
    for copy in copies:
        copy.wait()


def arrange(n_f, n_t, block, owner, hidden, exponents, in_cols, out_rows, slab):
    here = hidden.shape[0]
    blocks = slab // block
    whole = pl.BlockSpec(memory_space=VMEM)
    small = pl.BlockSpec(memory_space=SMEM)
    return pl.pallas_call(
        partial(arrange_kernel, n_f, n_t, block),
        out_shape=(
            jax.ShapeDtypeStruct((n_f, SPLIT, here // (n_t * SPLIT), slab), hidden.dtype),
            jax.ShapeDtypeStruct((2, here, slab), hidden.dtype),
            jax.ShapeDtypeStruct((blocks + -blocks % 8, in_cols), jnp.float32),
            jax.ShapeDtypeStruct((out_rows // block + -(out_rows // block) % 8, slab), jnp.float32),
            jax.ShapeDtypeStruct((n_f,), jnp.int32),
        ),
        in_specs=[small] + [pl.BlockSpec(memory_space=pl.ANY)] * 5,
        out_specs=(whole, whole, whole, whole, small),
        scratch_shapes=[VMEM(e.shape, e.dtype) for e in exponents]
        + [DMA((n_f + 1, SPLIT)), DMA((len(exponents),))],
        name="arrange",
    )(owner, *exponents, hidden)


def scale_in_place(w_scr, fac_ref, block):
    for b in range(w_scr.shape[0] // block):
        rows = slice(b * block, (b + 1) * block)
        for c in range(0, fac_ref.shape[1], block):
            cols = slice(c, c + block)
            weight = w_scr[rows, cols].astype(jnp.float32)
            w_scr[rows, cols] = (weight * fac_ref[b : b + 1, cols]).astype(jnp.bfloat16)


def attend_tile(scale, i, here, q_ref, kv_ref):
    query = q_ref[span_at(i, here), :]

    def chunk(at, state, masked):
        row_max, row_sum, accum = state
        scores = lax.dot_general(
            query, kv_ref[0, at, :], (((1,), (1,)), ((), ())), preferred_element_type=jnp.float32
        )
        if masked:
            q_pos = lax.broadcasted_iota(jnp.int32, scores.shape, 0)
            k_pos = lax.broadcasted_iota(jnp.int32, scores.shape, 1)
            scores = jnp.where(q_pos >= k_pos, scores, neg_large)
        new_max = jnp.maximum(row_max, jnp.max(scores, axis=1, keepdims=True))
        rescale = jnp.exp2((row_max - new_max) * scale)
        weights = jnp.exp2((scores - new_max) * scale)
        row_sum = row_sum * rescale + jnp.sum(weights, axis=1, keepdims=True)
        accum = accum * rescale + jnp.dot(
            weights.astype(jnp.bfloat16), kv_ref[1, at, :], preferred_element_type=jnp.float32
        )
        return (new_max, row_sum, accum)

    state = (
        jnp.full((here, 1), neg_large, jnp.float32),
        jnp.zeros((here, 1), jnp.float32),
        jnp.zeros((here, HD), jnp.float32),
    )
    state = chunk(span_at(i, here), state, True)
    wide = SPAN * here
    left = lax.rem(i, SPAN)
    state = lax.fori_loop(0, left, lambda j, s: chunk(span_at(i - 1 - j, here), s, False), state)
    _, row_sum, accum = lax.fori_loop(
        0, i // SPAN, lambda j, s: chunk(span_at(j, wide), s, False), state
    )
    return (accum / row_sum).astype(jnp.bfloat16)


SPAN = 4
PROJECT = 2
PAIR = PROJECT + 1
CLOSE = PAIR + LINE - 1
ATTEND = CLOSE + 1


def layer_kernel(
    n_f, n_t, share, block, inverse_ref, pieces, pair_ref, wq_ref, wk_ref, wv_ref, wo_ref,
    fac_ref, faco_ref, out_ref,
    w_scr, wo_scr, hid, mine, px, up_in, down_in, acc, q_scr, kv_scr,
    ctx, y, half_in, full_in, total, slabs_even, slabs_odd, fin, load,
    hid_send, hid_recv, side_send, pair_send, pair_recv,
    up_send, up_recv, down_send, down_recv, kv_send, kv_recv,
    line_send, line_recv, sum_send, sum_recv, slab_send, slab_recv, last_send, last_recv,
):
    f = lax.axis_index("fsdp")
    t = lax.axis_index("tp")
    n_z = n_f // CORES
    z, core = f // CORES, lax.rem(f, CORES)
    partner = z * CORES + (CORES - 1 - core)
    above, below = lax.rem(f + CORES, n_f), lax.rem(f - CORES + n_f, n_f)
    n_b = n_f * SPLIT
    here, slab = pair_ref.shape[1] // SPLIT, pair_ref.shape[2]
    quarter = here // n_t
    part = here // share
    per = n_f // n_t
    q_cols, k_cols = wq_ref.shape[1], wk_ref.shape[1]
    scale = 1.0 / (math.sqrt(HD) * math.log(2.0))
    side = [lax.rem(t + k, n_t) for k in range(n_t)]
    along = [t + 1 - 2 * lax.rem(t, 2), lax.rem(t + n_t // 2, n_t)]
    across = n_t - 1 - t
    group, mate = f // share, lax.rem(f, share)
    slabs = (slabs_even, slabs_odd)

    def piece_copy(i, p):
        b = f * SPLIT + p
        rows = span_at(t, quarter)
        return remote(
            pieces.at[i, p], hid.at[b, rows], hid_send.at[i, p], hid_recv.at[b, t], {"fsdp": i}
        )

    def beside_copy(p):
        b = f * SPLIT + p
        rows = slice(p * here, (p + 1) * here)
        return remote(
            pair_ref.at[1, rows], hid.at[b], hid_send.at[partner, p], hid_recv.at[b, 0],
            {"fsdp": partner},
        )

    def side_copy(b, k):
        rows = span_at(t, quarter)
        return remote(
            hid.at[b, rows], hid.at[b, rows], side_send.at[b, k], hid_recv.at[b, t], {"tp": side[k]}
        )

    def pair_copy(b):
        return remote(
            mine.at[lax.rem(b, 2), CORES - 1 - core], px.at[b], pair_send.at[b], pair_recv.at[b],
            {"fsdp": partner},
        )

    def up_copy(b, zz):
        return remote(
            px.at[b, zz], up_in.at[b, zz], up_send.at[b, zz], up_recv.at[b, zz], {"fsdp": above}
        )

    def down_copy(b, zz):
        return remote(
            px.at[b, zz], down_in.at[b, zz], down_send.at[b, zz], down_recv.at[b, zz],
            {"fsdp": below},
        )

    def kv_copy(b, source, k):
        rows = pl.ds(pl.multiple_of(b * here + source * part, part), part)
        return remote(
            kv_scr.at[:, rows], kv_scr.at[:, rows], kv_send.at[b, k], kv_recv.at[b, source],
            {"fsdp": group * share + lax.rem(mate + k, share)},
        )

    def line_copy(i, zz, to, which):
        rows = span_at(i, here)
        h = lax.rem(zz + n_z, n_z) * CORES + core
        return remote(
            ctx.at[h, rows], ctx.at[h, rows], line_send.at[i, h // CORES, which],
            line_recv.at[i, h], {"fsdp": to},
        )

    def line_wait(i, h):
        rows = span_at(i, here)
        remote(
            ctx.at[h, rows], ctx.at[h, rows], line_send.at[i, 0, 0], line_recv.at[i, h],
            {"fsdp": partner},
        ).wait_recv()

    def diagonal_copy(i):
        return remote(
            y.at[i, across], half_in.at[i], sum_send.at[i, 2], sum_recv.at[i, 2],
            {"tp": across},
        )

    def full_copy(i, k):
        return remote(
            y.at[i, along[k]], full_in.at[i, k], sum_send.at[i, k], sum_recv.at[i, k],
            {"tp": along[k]},
        )

    def slab_copy(i, p):
        return remote(
            total.at[i], slabs[p].at[f], slab_send.at[i], slab_recv.at[f, p], {"fsdp": i // SPLIT}
        )

    def out_rows(p, source):
        return pl.ds(pl.multiple_of(p * here + source * quarter, quarter), quarter)

    def last_copy(p, k):
        return remote(
            fin.at[p, side[k]], out_ref.at[out_rows(p, t)], last_send.at[p, k - 1],
            last_recv.at[p, k - 1], {"tp": side[k]},
        )

    loads = [
        pltpu.make_async_copy(wq_ref, w_scr.at[:, :q_cols], load.at[0]),
        pltpu.make_async_copy(wk_ref, w_scr.at[:, q_cols : q_cols + k_cols], load.at[1]),
        pltpu.make_async_copy(wv_ref, w_scr.at[:, q_cols + k_cols :], load.at[2]),
        pltpu.make_async_copy(wo_ref, wo_scr.at[:, :slab], load.at[3]),
    ]
    for copy in loads:
        copy.start()
    greet_all(n_f, n_t, f, t)
    for p in range(SPLIT):
        beside_copy(p).start()
    for p in range(SPLIT):
        for d in range(n_z - 1, 0, -1):
            for c in range(CORES):

                @pl.when(z + d < n_z)
                def _():
                    piece_copy(lax.rem((z + d) * CORES + c, n_f), p).start()

                @pl.when(z - d >= 0)
                def _():
                    piece_copy(lax.rem((z - d + n_z) * CORES + c, n_f), p).start()

    for p in range(SPLIT):
        hid[f * SPLIT + p] = pair_ref[0, p * here : (p + 1) * here]
    wo_scr[:, slab:] = jnp.zeros((wo_scr.shape[0], wo_scr.shape[1] - slab), jnp.bfloat16)
    for copy in loads:
        copy.wait()
    scale_in_place(w_scr, fac_ref, block)
    scale_in_place(wo_scr, faco_ref, block)

    def piece_like(b, source):
        rows = span_at(source, quarter)
        return remote(
            pieces.at[0, 0], hid.at[b, rows], hid_send.at[0, 0], hid_recv.at[b, source],
            {"fsdp": above},
        )

    def pass_on(b):
        piece_like(b, t).wait_recv()
        for k in range(1, n_t):
            side_copy(b, k).start()

    def project(b):
        @pl.when(b // SPLIT == partner)
        def _():
            remote(
                pair_ref.at[1, :here], hid.at[b], hid_send.at[0, 0], hid_recv.at[b, 0],
                {"fsdp": partner},
            ).wait_recv()

        @pl.when(b // (SPLIT * CORES) != z)
        def _():
            for k in range(1, n_t):
                piece_like(b, side[k]).wait_recv()

        @pl.when(b >= 2)
        def _():
            pair_copy(b - 2).wait_send()

        both = jnp.dot(hid[b], w_scr[...], preferred_element_type=jnp.float32).astype(
            jnp.bfloat16
        )
        for j in range(n_f):
            g, p = j // share, j % share
            spot = mine.at[lax.rem(b, 2), j % CORES, j // CORES]
            spot[:here, :] = both[:, j * HD : (j + 1) * HD]
            rows = slice(p * part, (p + 1) * part)
            k_at = q_cols + g * HD
            v_at = q_cols + k_cols + g * HD
            spot[here : here + part, :] = both[rows, k_at : k_at + HD]
            spot[here + part :, :] = both[rows, v_at : v_at + HD]
        pair_copy(b).start()

    def join_pair(b):
        pair_copy(b).wait_recv()
        for zz in range(n_z):
            px[b, zz] = (
                px[b, zz].astype(jnp.float32) + mine[lax.rem(b, 2), core, zz].astype(jnp.float32)
            ).astype(jnp.bfloat16)

    def close(b):
        acc[...] = px[b, z].astype(jnp.float32)

        @pl.when(z > 0)
        def _():
            up_copy(b, z).wait_recv()
            acc[...] += up_in[b, z].astype(jnp.float32)

        @pl.when(z < n_z - 1)
        def _():
            down_copy(b, z).wait_recv()
            acc[...] += down_in[b, z].astype(jnp.float32)

        q_scr[span_at(b, here), :] = acc[:here, :].astype(jnp.bfloat16)
        rows = pl.ds(pl.multiple_of(b * here + mate * part, part), part)
        kv_scr[0, rows, :] = acc[here : here + part, :].astype(jnp.bfloat16)
        kv_scr[1, rows, :] = acc[here + part :, :].astype(jnp.bfloat16)
        for k in range(1, share):
            kv_copy(b, mate, k).start()

    def relay(s, d):
        @pl.when(within(s - ATTEND - d, n_b))
        def _():
            i = s - ATTEND - d

            @pl.when(z - d >= 0)
            def _():
                zz = lax.rem(z - d + n_z, n_z)
                line_wait(i, zz * CORES + core)

                @pl.when(z < n_z - 1)
                def _():
                    line_copy(i, zz, above, 1).start()

                line_copy(i, zz, partner, 0).start()

            @pl.when(z + d < n_z)
            def _():
                zz = lax.rem(z + d, n_z)
                line_wait(i, zz * CORES + core)

                @pl.when(z > 0)
                def _():
                    line_copy(i, zz, below, 2).start()

                line_copy(i, zz, partner, 0).start()

    def step(s, carry):
        @pl.when(within(s, n_b))
        def _():
            @pl.when(s // (SPLIT * CORES) != z)
            def _():
                pass_on(s)

        @pl.when(within(s - PAIR, n_b))
        def _():
            join_pair(s - PAIR)

        up_at = s - PAIR - z

        @pl.when(within(up_at, n_b))
        def _():
            b = up_at
            for zz in range(n_z - 1, 0, -1):

                @pl.when(zz > z)
                def _():
                    @pl.when(z > 0)
                    def _():
                        up_copy(b, zz).wait_recv()
                        px[b, zz] = (
                            px[b, zz].astype(jnp.float32) + up_in[b, zz].astype(jnp.float32)
                        ).astype(jnp.bfloat16)

                    up_copy(b, zz).start()

        down_at = s - PAIR - (n_z - 1 - z)

        @pl.when(within(down_at, n_b))
        def _():
            b = down_at
            for zz in range(n_z - 1):

                @pl.when(zz < z)
                def _():
                    @pl.when(z < n_z - 1)
                    def _():
                        down_copy(b, zz).wait_recv()
                        px[b, zz] = (
                            px[b, zz].astype(jnp.float32) + down_in[b, zz].astype(jnp.float32)
                        ).astype(jnp.bfloat16)

                    down_copy(b, zz).start()

        @pl.when(within(s - PROJECT, n_b))
        def _():
            project(s - PROJECT)

        @pl.when(within(s - CLOSE, n_b))
        def _():
            close(s - CLOSE)

        @pl.when(within(s - ATTEND, n_b))
        def _():
            i = s - ATTEND
            for k in range(1, share):
                kv_copy(i, lax.rem(mate - k + share, share), k).wait_recv()
            ctx[f, span_at(i, here), :] = attend_tile(scale, i, here, q_scr, kv_scr)

            @pl.when(z < n_z - 1)
            def _():
                line_copy(i, z, above, 1).start()

            @pl.when(z > 0)
            def _():
                line_copy(i, z, below, 2).start()

            line_copy(i, z, partner, 0).start()

        for d in range(1, n_z):
            relay(s, d)

        @pl.when(within(s - ATTEND - n_z, n_b))
        def _():
            i = s - ATTEND - n_z
            for zz in range(n_z):
                line_wait(i, zz * CORES + (CORES - 1 - core))
            context = jnp.concatenate([ctx[h, span_at(i, here)] for h in range(n_f)], axis=1)
            part = jnp.dot(context, wo_scr[...], preferred_element_type=jnp.float32).astype(
                jnp.bfloat16
            )
            for r in range(n_t):
                y[i, r] = part[r * quarter : (r + 1) * quarter, :slab]
            diagonal_copy(i).start()
            for k in range(2):
                full_copy(i, k).start()

        @pl.when(within(s - ATTEND - n_z - 1, n_b))
        def _():
            i = s - ATTEND - n_z - 1
            diagonal_copy(i).wait_recv()
            summed = y[i, t].astype(jnp.float32) + half_in[i].astype(jnp.float32)
            for k in range(2):
                full_copy(i, k).wait_recv()
                summed = summed + full_in[i, k].astype(jnp.float32)
            total[i] = summed.astype(jnp.bfloat16)

            for p in range(SPLIT):

                @pl.when(i == f * SPLIT + p)
                def _():
                    slabs[p][f] = total[i]

                @pl.when(jnp.logical_and(i // SPLIT != f, lax.rem(i, SPLIT) == p))
                def _():
                    slab_copy(i, p).start()

        for p in range(SPLIT):

            @pl.when(s - ATTEND - n_z - 2 == f * SPLIT + p)
            def _():
                for d in range(1, n_f):
                    source = lax.rem(f + d, n_f)
                    remote(
                        total.at[0], slabs[p].at[source], slab_send.at[0], slab_recv.at[source, p],
                        {"fsdp": source},
                    ).wait_recv()
                for j in range(n_f):
                    cols = slice((j % per) * slab, (j % per + 1) * slab)
                    fin[p, j // per, :, cols] = slabs[p][inverse_ref[j]]
                for k in range(1, n_t):
                    last_copy(p, k).start()
                out_ref[out_rows(p, t), :] = fin[p, t]

        return carry

    lax.fori_loop(0, n_b + ATTEND + n_z + 2, step, 0)

    def finish_head(b, carry):
        for k in range(1, share):
            kv_copy(b, mate, k).wait_send()
        @pl.when(b >= n_b - 2)
        def _():
            pair_copy(b).wait_send()

        @pl.when(b // (SPLIT * CORES) != z)
        def _():
            piece_copy(b // SPLIT, lax.rem(b, SPLIT)).wait_send()
            for k in range(1, n_t):
                side_copy(b, k).wait_send()

        for zz in range(n_z):

            @pl.when(zz > z)
            def _():
                up_copy(b, zz).wait_send()

            @pl.when(zz < z)
            def _():
                down_copy(b, zz).wait_send()

        return carry

    lax.fori_loop(0, n_b, finish_head, 0)
    for p in range(SPLIT):
        beside_copy(p).wait_send()


    def finish(i, carry):
        @pl.when(i // SPLIT != f)
        def _():
            slab_copy(i, 0).wait_send()

        diagonal_copy(i).wait_send()
        for k in range(2):
            full_copy(i, k).wait_send()
        for zz in range(n_z):
            line_copy(i, zz, partner, 0).wait_send()

            @pl.when(jnp.logical_and(zz <= z, z < n_z - 1))
            def _():
                line_copy(i, zz, above, 1).wait_send()

            @pl.when(jnp.logical_and(zz >= z, z > 0))
            def _():
                line_copy(i, zz, below, 2).wait_send()

        return carry

    lax.fori_loop(0, n_b, finish, 0)
    for p in range(SPLIT):
        for k in range(1, n_t):
            source = lax.rem(t - k + n_t, n_t)
            remote(
                fin.at[p, 0], out_ref.at[out_rows(p, source)], last_send.at[p, k - 1],
                last_recv.at[p, k - 1], {"tp": side[1]},
            ).wait_recv()
            last_copy(p, k).wait_send()


def layer(n_f, n_t, share, block, inverse, pieces, pair, w_query, w_key, w_value, w_out, fac, faco):
    n_b = n_f * SPLIT
    here, slab = pair.shape[1] // SPLIT, pair.shape[2]
    quarter = here // n_t
    n_z = n_f // CORES
    cols = w_query.shape[1] + 2 * w_key.shape[1]
    packed = here + 2 * (here // share)
    tokens = here * n_b
    wide = slab * n_f // n_t
    whole = pl.BlockSpec(memory_space=VMEM)
    stay = pl.BlockSpec(memory_space=pl.ANY)
    small = jnp.bfloat16
    return pl.pallas_call(
        partial(layer_kernel, n_f, n_t, share, block),
        out_shape=jax.ShapeDtypeStruct((here * SPLIT, wide), small),
        in_specs=[pl.BlockSpec(memory_space=SMEM), whole, whole] + [stay] * 4 + [whole] * 2,
        out_specs=whole,
        scratch_shapes=[
            VMEM((slab, cols), small),
            VMEM((w_out.shape[0], slab + -slab % 256), small),
            VMEM((n_b, here, slab), small),
            VMEM((2, CORES, n_z, packed, HD), small),
            VMEM((n_b, n_z, packed, HD), small),
            VMEM((n_b, n_z, packed, HD), small),
            VMEM((n_b, n_z, packed, HD), small),
            VMEM((packed, HD), jnp.float32),
            VMEM((tokens, HD), small),
            VMEM((2, tokens, HD), small),
            VMEM((n_f, tokens, HD), small),
            VMEM((n_b, n_t, quarter, slab), small),
            VMEM((n_b, quarter, slab), small),
            VMEM((n_b, 2, quarter, slab), small),
            VMEM((n_b, quarter, slab), small),
            VMEM((n_f, quarter, slab), small),
            VMEM((n_f, quarter, slab), small),
            VMEM((SPLIT, n_t, quarter, wide), small),
            DMA((4,)),
            DMA((n_f, SPLIT)),
            DMA((n_b, n_t)),
            DMA((n_b, n_t)),
            DMA((n_b,)),
            DMA((n_b,)),
            DMA((n_b, n_z)),
            DMA((n_b, n_z)),
            DMA((n_b, n_z)),
            DMA((n_b, n_z)),
            DMA((n_b, share)),
            DMA((n_b, share)),
            DMA((n_b, n_z, 3)),
            DMA((n_b, n_f)),
            DMA((n_b, 3)),
            DMA((n_b, 3)),
            DMA((n_b,)),
            DMA((n_f, SPLIT)),
            DMA((SPLIT, n_t - 1)),
            DMA((SPLIT, n_t - 1)),
        ],
        compiler_params=pltpu.CompilerParams(
            collective_id=0, has_side_effects=True, vmem_limit_bytes=67043328
        ),
        name="layer",
    )(inverse, pieces, pair, w_query, w_key, w_value, w_out, fac, faco)


def stationary_body(
    n_f, n_t, hidden, w_query, w_key, w_value, w_out, exp_query, exp_key, exp_value, exp_out, owner
):
    slab = w_query.shape[0]
    block = hidden.shape[1] // exp_query.shape[0]
    q_cols, k_cols = w_query.shape[1], w_key.shape[1]
    pieces, pair, fac, faco, inverse = arrange(
        n_f, n_t, block, owner, hidden, (exp_query.T, exp_key.T, exp_value.T, exp_out),
        q_cols + 2 * k_cols, w_out.shape[0], slab,
    )
    return layer(
        n_f, n_t, q_cols // k_cols, block, inverse, pieces, pair, w_query, w_key, w_value, w_out,
        fac, faco,
    )


def solution(mesh):
    n_f, n_t = mesh.shape["fsdp"], mesh.shape["tp"]

    def body(*arrays):
        hidden, w_query, w_key = arrays[0], arrays[1], arrays[2]
        heads, kv_heads = w_query.shape[1] // HD, w_key.shape[1] // HD
        share = heads // kv_heads
        fits = (
            heads == n_f
            and n_t == SIDE * SIDE
            and n_f % n_t == 0
            and n_f == LINE * CORES
            and hidden.shape[0] % (16 * SPLIT * n_t) == 0
            and hidden.shape[0] % (16 * SPLIT * share) == 0
        )
        if fits:
            return stationary_body(n_f, n_t, *arrays)
        return gather_body(*arrays)

    placed = (
        P("fsdp", None),
        P("fsdp", "tp"),
        P("fsdp", "tp"),
        P("fsdp", "tp"),
        P("tp", "fsdp"),
        P(),
        P(),
        P(),
        P(),
        P(),
    )
    return jax.shard_map(
        body, mesh=mesh, in_specs=placed, out_specs=P("fsdp", "tp"), check_vma=False
    )
```
